32 devices in a mesh: gx: 4 (over z), gy: 2 (over x), gz: 4 (over y, core).
Axes of the slice: x: 2, y: 2, z: 4, core: 2. Of those that a mesh axis runs over, the one named last changes fastest.
Arguments:
- bases: float32 [4, 2, 4, 1024, 128], P('gx', 'gy', 'gz'), may hold values from -1 to 1, as said below
- ranks: int32 [4, 2, 4], P('gx', 'gy', 'gz'), may hold values from 64 to 128
- couplings: bfloat16 [4, 2, 4, 5, 1024, 1024], P('gx', 'gy', 'gz'), may hold values from -6 to 6
- vectors: float32 [4, 2, 4, 1024, 256], P('gx', 'gy', 'gz'), may hold values from -0.1875 to 0.1875
Outputs:
- projected: float32 [4, 2, 4, 5, 128, 128], P('gx', 'gy', 'gz')
- applied: float32 [4, 2, 4, 1024, 256], P('gx', 'gy', 'gz')
The draws below stay inside these ranges and needn't reach their ends.
Inputs may be any that keep to these rules, and one draw needn't show every extreme that they name: `bases`: for each subdomain the 1024 x 128 matrix has orthonormal columns.
All inputs are finite; a program needn't handle non-finite values.
Results may differ from the reference program's by a relative error of at most 0.0003.
Values sent between devices are 32-bit elements; how exact they have to be, the bound alone decides.
A program may use at most 64 MiB of HBM per device.

```python
import jax
import jax.numpy as jnp
from jax import lax

M = 1024
K = 128
R = 256
NB = 5
N_GX = 4
N_GY = 2
N_GZ = 4


def orthonormal_columns(sample):
    return jnp.linalg.qr(sample)[0]


def draw_bases(key, part):
    device_total = N_GX * N_GY * N_GZ
    sample = jax.random.normal(key, (device_total, M, K), jnp.float32)
    orthonormal = jax.vmap(orthonormal_columns)(sample)
    return orthonormal.reshape(N_GX, N_GY, N_GZ, M, K).astype(jnp.float32)


def touch_ends(array, stream_key, least, top_value):
    longest = array.shape.index(max(array.shape))
    spots = []
    for shift in (0, 1):
        where = [jax.random.randint(jax.random.fold_in(stream_key, axis), (), 0, length) for axis, length in enumerate(array.shape)]
        where[longest] = (where[longest] + shift) % array.shape[longest]
        spots.append(tuple(where))
    return array.at[spots[0]].set(least).at[spots[1]].set(top_value)


def steps_of(rng, shape, split, low, top_value):
    def one(dim, parts):
        heights = jax.random.uniform(jax.random.fold_in(jax.random.fold_in(rng, 6), dim), (parts,), jnp.float32, low / len(split), top_value / len(split))
        return jnp.repeat(jnp.exp(heights), shape[dim] // parts).reshape((-1,) + (1,) * (len(shape) - dim - 1))

    gain = one(*split[0])
    for cut in split[1:]:
        gain = gain * one(*cut)
    return gain


def normal_values(own_key, extent, deviation, bound, pieces=(), kind=jnp.bfloat16):
    drawn = deviation * jax.random.normal(own_key, extent, jnp.float32)
    if pieces:
        drawn = drawn * steps_of(own_key, extent, pieces, -0.22, 0.18)
    return jnp.clip(drawn, -bound, bound).astype(kind)


def setup_inputs(seed: int = 0) -> dict:
    seeds = jax.random.split(jax.random.key(seed), 5)
    return {
        "bases": draw_bases(jax.random.fold_in(seeds[4], 71), 0),
        "ranks": touch_ends(jax.random.randint(seeds[1], (N_GX, N_GY, N_GZ), K // 2, K + 1), jax.random.fold_in(seeds[1], 1), K // 2, K).astype(jnp.int32),
        "couplings": normal_values(seeds[2], (N_GX, N_GY, N_GZ, NB, M, M), 1.0, 6.0, ((0, 4), (1, 2), (2, 4))),
        "vectors": normal_values(seeds[3], (N_GX, N_GY, N_GZ, M, R), M ** -0.5, 0.1875, ((0, 4), (1, 2), (2, 4)), jnp.float32),
    }


OFFSET_LIST = ((1, 0, 0), (0, 1, 0), (0, 0, 1), (1, 1, 0), (1, 0, 1), (0, 1, 1), (1, 1, 1))

def reference(bases, ranks, couplings, vectors):
    columns = jnp.arange(K, dtype=jnp.int32)
    keep = (columns < ranks[..., None]).astype(jnp.float32)
    masked = bases * keep[..., None, :]
    joined = jnp.concatenate([masked, vectors], axis=-1)
    padded = jnp.pad(joined, ((0, 1), (0, 1), (0, 1), (0, 0), (0, 0)))
    device_total = N_GX * N_GY * N_GZ
    neighbour_list = []
    for slot in range(NB):
        shift_x, shift_y, shift_z = OFFSET_LIST[slot]
        moved = padded[shift_x:shift_x + N_GX, shift_y:shift_y + N_GY, shift_z:shift_z + N_GZ]
        neighbour_list.append(moved.reshape(device_total, M, K + R))
    neighbours = jnp.stack(neighbour_list, axis=1)
    flat_bases = masked.reshape(device_total, M, K)
    flat_couplings = couplings.reshape(device_total, NB, M, M)

    def one_device(index):
        own_basis = flat_bases[index]

        def one_block(slot):
            neighbour = neighbours[index, slot]
            coupling = flat_couplings[index, slot].astype(jnp.float32)
            coupled = jnp.dot(coupling, neighbour[:, :K], precision=lax.Precision.HIGHEST)
            acted = jnp.dot(coupling, neighbour[:, K:], precision=lax.Precision.HIGHEST)
            return (jnp.dot(own_basis.T, coupled, precision=lax.Precision.HIGHEST), acted)
        blocks, acted = lax.map(one_block, jnp.arange(NB, dtype=jnp.int32))
        return (blocks, jnp.sum(acted, axis=0))
    result, applied = lax.map(one_device, jnp.arange(device_total, dtype=jnp.int32))
    return (result.reshape(N_GX, N_GY, N_GZ, NB, K, K), applied.reshape(N_GX, N_GY, N_GZ, M, R))
```

```python
import functools

import jax
import jax.numpy as jnp
from jax import lax
from jax.experimental import pallas as pl
from jax.experimental.pallas import tpu as pltpu
from jax.sharding import PartitionSpec as P

OFFSET_LIST = ((1, 0, 0), (0, 1, 0), (0, 0, 1), (1, 1, 0), (1, 0, 1), (0, 1, 1), (1, 1, 1))
AXES = ("gx", "gy", "gz")
X, Y, Z, XY, XZ = range(5)
LEFT_ORDER = (XY, Y, X, XZ, Z)
LEFT_SLOTS = (X, Y, Z, XZ)


def split2(value):
    high = value.astype(jnp.bfloat16)
    low = (value - high.astype(jnp.float32)).astype(jnp.bfloat16)
    return high, low


def dot32(left, right):
    return jnp.dot(left, right, preferred_element_type=jnp.float32)


def kernel(
    sizes, ranks_ref, bases_ref, couplings_ref, vectors_ref, projected_ref, applied_ref,
    basis, stacked, basis_parts, blocks, values, left_out, left_in, relay, back_out,
    ready, basis_sem, block_sem, value_send, value_recv, left_send, left_recv, relay_send, relay_recv,
    back_send, back_recv,
):
    count, m, k = blocks.shape[0], basis.shape[0], basis.shape[1]
    r = applied_ref.shape[1]
    half = m // 2
    place = [lax.axis_index(name) for name in AXES]
    has_up = [p < n - 1 for p, n in zip(place, sizes)]
    has_down = [p > 0 for p in place]

    def every(flags, offset):
        out = None
        for flag, o in zip(flags, offset):
            if o:
                out = flag if out is None else jnp.logical_and(out, flag)
        return out

    up = [every(has_up, o) for o in OFFSET_LIST[:count]]
    down = [every(has_down, o) for o in OFFSET_LIST[:count]]

    def device(offset, sign):
        return {name: p + sign * o for name, p, o in zip(AXES, place, offset)}

    barrier = pltpu.get_barrier_semaphore()
    partners = jnp.int32(0)
    for s in range(count):
        partners = partners + down[s].astype(jnp.int32)

        @pl.when(up[s])
        def _():
            pl.semaphore_signal(
                barrier, inc=1, device_id=device(OFFSET_LIST[s], 1), device_id_type=pl.DeviceIdType.MESH
            )

    @pl.when(partners > 0)
    def _():
        pl.semaphore_wait(barrier, partners)

    def rows(part):
        return pl.ds(part * half, half)

    def remote(src, dst, send, recv, offset, sign):
        return pltpu.make_async_remote_copy(
            src_ref=src, dst_ref=dst, send_sem=send, recv_sem=recv,
            device_id=device(offset, sign), device_id_type=pl.DeviceIdType.MESH,
        )

    def value_copy(slot, piece, source, offset):
        return remote(
            source.at[piece], values.at[slot, piece],
            value_send.at[slot, len(sent[slot])], value_recv.at[slot, len(sent[slot])], offset, -1,
        )

    def pieces(part, total):
        return [pl.ds(part * half + p * (half // total), half // total) for p in range(total)]

    sent = {s: [] for s in range(count)}

    def plan(slot, part, source, offset, flag, total=1):
        for piece in pieces(part, total):
            sent[slot].append((value_copy(slot, piece, source, offset), piece, flag, part))

    for s in (X, Y, Z):
        for part in (0, 1):
            plan(s, part, vectors_ref, OFFSET_LIST[s], down[s])
    plan(XY, 0, values.at[X], OFFSET_LIST[Y], jnp.logical_and(has_up[0], has_down[1]), 2)
    plan(XY, 1, values.at[Y], OFFSET_LIST[X], jnp.logical_and(has_up[1], has_down[0]), 2)
    for part in (0, 1):
        plan(XZ, part, values.at[X], OFFSET_LIST[Z], jnp.logical_and(has_up[0], has_down[2]))

    def start(slot, part):
        for copy, _, flag, its in sent[slot]:
            if its == part:
                pl.when(flag)(copy.start)

    def arrived(slot, n):
        pl.when(up[slot])(sent[slot][n][0].wait_recv)

    relays = [
        remote(left_out.at[XY, part], relay.at[part], relay_send.at[part], relay_recv.at[part], OFFSET_LIST[s], 1)
        for part, s in ((0, X), (1, Y))
    ]
    onward = [
        remote(relay.at[part], left_in.at[XY, part], left_send.at[XY, part], left_recv.at[XY, part], OFFSET_LIST[s], 1)
        for part, s in ((0, Y), (1, X))
    ]
    passed = (
        ((relays[0], onward[0]), jnp.logical_and(has_down[0], has_up[1])),
        ((relays[1], onward[1]), jnp.logical_and(has_down[1], has_up[0])),
    )
    left_copies = [
        relays if s == XY else [
            remote(left_out.at[s], left_in.at[s], left_send.at[s, 0], left_recv.at[s, 0], OFFSET_LIST[s], 1)
        ]
        for s in range(count)
    ]
    back_copies = [
        remote(back_out.at[s], projected_ref.at[s], back_send.at[s], back_recv.at[s], OFFSET_LIST[s], -1)
        for s in range(count)
    ]

    start(X, 0)
    start(Y, 1)
    start(Z, 0)
    start(X, 1)
    start(Y, 0)
    start(Z, 1)

    for s in LEFT_SLOTS:
        @pl.when(down[s])
        def _():
            pl.semaphore_signal(
                ready.at[s], inc=1, device_id=device(OFFSET_LIST[s], -1), device_id_type=pl.DeviceIdType.MESH
            )

    basis_copy = pltpu.make_async_copy(bases_ref, basis, basis_sem)
    basis_copy.start()
    block_copies = [
        pltpu.make_async_copy(couplings_ref.at[s], blocks.at[s], block_sem.at[s]) for s in range(count)
    ]
    for s in LEFT_ORDER:
        block_copies[s].start()

    basis_copy.wait()
    columns = lax.broadcasted_iota(jnp.int32, (m, k), 1)
    masked = jnp.where(columns < ranks_ref[0, 0, 0], basis[...], 0.0)
    high, low = split2(masked)
    basis_parts[:, :k] = high
    basis_parts[:, k:] = low
    high, low = split2(masked.T)
    stacked[:k] = high
    stacked[k:] = low

    for s in LEFT_SLOTS:
        @pl.when(up[s])
        def _():
            pl.semaphore_wait(ready.at[s], 1)

    for s in LEFT_ORDER:
        block_copies[s].wait()

        @pl.when(up[s])
        def _():
            @pl.loop(0, 2)
            def _(part):
                there = pl.ds(pl.multiple_of(part * half, half), half)
                both = dot32(stacked[...], blocks[s, :, there])
                left_out[s, part] = both[:k] + both[k:]

            if s != XZ:
                for copy in left_copies[s]:
                    copy.start()

    applied_ref[...] = jnp.zeros_like(applied_ref)
    for s in range(count):

        @pl.when(jnp.logical_not(up[s]))
        def _():
            projected_ref[s] = jnp.zeros((k, k), jnp.float32)

    for copy, flag in passed:
        @pl.when(flag)
        def _():
            copy[0].wait_recv()
            copy[1].start()

    pl.when(up[XZ])(left_copies[XZ][0].start)

    tall = min(512, m)

    def apply(slot, n):
        piece = sent[slot][n][1]

        @pl.when(up[slot])
        def _():
            high, low = split2(values[slot, piece])
            pair = jnp.concatenate([high, low], axis=1)

            @pl.loop(0, m // tall)
            def _(step):
                there = pl.ds(pl.multiple_of(step * tall, tall), tall)
                both = dot32(blocks[slot, there, piece], pair)
                applied_ref[there] += both[:, :r] + both[:, r:]

    def project(slot):
        @pl.when(down[slot])
        def _():
            for copy in onward if slot == XY else left_copies[slot]:
                copy.wait_recv()
            out = None
            for part in (0, 1):
                high, low = split2(left_in[slot, part])
                first = dot32(high, basis_parts[rows(part)])
                term = first[:, :k] + first[:, k:] + dot32(low, basis_parts[rows(part), :k])
                out = term if out is None else out + term
            back_out[slot] = out
            back_copies[slot].start()

    arrived(Z, 0)
    apply(Z, 0)
    arrived(X, 0)
    start(XY, 0)
    start(XZ, 0)
    arrived(Y, 1)
    start(XY, 1)
    arrived(Z, 1)
    apply(Z, 1)
    apply(X, 0)
    apply(Y, 1)
    project(Z)
    arrived(XZ, 0)
    apply(XZ, 0)
    project(Y)
    project(X)
    arrived(X, 1)
    start(XZ, 1)
    arrived(Y, 0)
    apply(X, 1)
    apply(Y, 0)
    arrived(XZ, 1)
    apply(XZ, 1)
    project(XY)
    for n in (0, 2):
        arrived(XY, n)
        apply(XY, n)
    project(XZ)
    for n in (1, 3):
        arrived(XY, n)
        apply(XY, n)
    for s in range(count):
        pl.when(up[s])(back_copies[s].wait_recv)
    for s in range(count):
        for copy, _, flag, _ in sent[s]:
            pl.when(flag)(copy.wait_send)
        for copy in left_copies[s]:
            pl.when(up[s])(copy.wait_send)
        pl.when(down[s])(back_copies[s].wait_send)
    for copy, flag in passed:
        pl.when(flag)(copy[1].wait_send)


def writer(projected_ref, applied_ref, projected_out, applied_out, sems):
    copies = [
        pltpu.make_async_copy(projected_ref, projected_out, sems.at[0]),
        pltpu.make_async_copy(applied_ref, applied_out, sems.at[1]),
    ]
    for copy in copies:
        copy.start()
    for copy in copies:
        copy.wait()


def solution(mesh):
    sizes = tuple(mesh.shape[name] for name in AXES)

    def local(bases, ranks, couplings, vectors):
        m, k = bases.shape[-2:]
        count = couplings.shape[3]
        r = vectors.shape[-1]
        f32, bf16 = jnp.float32, jnp.bfloat16
        dma = pltpu.SemaphoreType.DMA
        projected, applied = pl.pallas_call(
            functools.partial(kernel, sizes),
            out_shape=(
                pltpu.VMEM((count, k, k), f32),
                pltpu.VMEM((m, r), f32),
            ),
            in_specs=[pl.BlockSpec(memory_space=pltpu.SMEM)] + [pl.BlockSpec(memory_space=pltpu.HBM)] * 3,
            out_specs=(pl.BlockSpec(memory_space=pltpu.VMEM),) * 2,
            scratch_shapes=[
                pltpu.VMEM((m, k), f32),
                pltpu.VMEM((2 * k, m), bf16),
                pltpu.VMEM((m, 2 * k), bf16),
                pltpu.VMEM((count, m, m), bf16),
                pltpu.VMEM((count, m, r), f32),
                pltpu.VMEM((count, 2, k, m // 2), f32),
                pltpu.VMEM((count, 2, k, m // 2), f32),
                pltpu.VMEM((2, k, m // 2), f32),
                pltpu.VMEM((count, k, k), f32),
                pltpu.SemaphoreType.REGULAR((count,)),
                dma,
                dma((count,)),
                dma((count, 4)),
                dma((count, 4)),
                dma((count, 2)),
                dma((count, 2)),
                dma((2,)),
                dma((2,)),
                dma((count,)),
                dma((count,)),
            ],
            compiler_params=pltpu.CompilerParams(collective_id=0, has_side_effects=True, vmem_limit_bytes=64000 << 10),
        )(
            ranks,
            bases.reshape(m, k),
            couplings.reshape(count, m, m),
            vectors.reshape(m, r),
        )
        return (
            projected.reshape(1, 1, 1, count, k, k),
            applied.reshape(1, 1, 1, m, r),
        )

    return jax.shard_map(
        local,
        mesh=mesh,
        in_specs=(
            P("gx", "gy", "gz", None, None),
            P("gx", "gy", "gz"),
            P("gx", "gy", "gz", None, None, None),
            P("gx", "gy", "gz", None, None),
        ),
        out_specs=(P("gx", "gy", "gz", None, None, None), P("gx", "gy", "gz", None, None)),
        check_vma=False,
    )
```

```python
import functools

import jax
import jax.numpy as jnp
from jax import lax
from jax.experimental import pallas as pl
from jax.experimental.pallas import tpu as pltpu
from jax.sharding import PartitionSpec as P

OFFSET_LIST = ((1, 0, 0), (0, 1, 0), (0, 0, 1), (1, 1, 0), (1, 0, 1), (0, 1, 1), (1, 1, 1))
AXES = ("gx", "gy", "gz")
X, Y, Z, XY, XZ = range(5)
LEFT_ORDER = (XY, Y, X, XZ, Z)
LEFT_SLOTS = (X, Y, Z, XZ)


def split2(value):
    high = value.astype(jnp.bfloat16)
    low = (value - high.astype(jnp.float32)).astype(jnp.bfloat16)
    return high, low


def dot32(left, right):
    return jnp.dot(left, right, preferred_element_type=jnp.float32)


def kernel(
    sizes, ranks_ref, bases_ref, couplings_ref, vectors_ref, projected_ref, applied_ref,
    basis, stacked, basis_parts, blocks, values, left_out, left_in, relay, back_out,
    ready, basis_sem, block_sem, value_send, value_recv, left_send, left_recv, relay_send, relay_recv,
    back_send, back_recv,
):
    count, m, k = blocks.shape[0], basis.shape[0], basis.shape[1]
    r = applied_ref.shape[1]
    half = m // 2
    place = [lax.axis_index(name) for name in AXES]
    has_up = [p < n - 1 for p, n in zip(place, sizes)]
    has_down = [p > 0 for p in place]

    def every(flags, offset):
        out = None
        for flag, o in zip(flags, offset):
            if o:
                out = flag if out is None else jnp.logical_and(out, flag)
        return out

    up = [every(has_up, o) for o in OFFSET_LIST[:count]]
    down = [every(has_down, o) for o in OFFSET_LIST[:count]]

    def device(offset, sign):
        return {name: p + sign * o for name, p, o in zip(AXES, place, offset)}

    basis_copy = pltpu.make_async_copy(bases_ref, basis, basis_sem)
    basis_copy.start()

    barrier = pltpu.get_barrier_semaphore()
    partners = jnp.int32(0)
    for s in range(count):
        partners = partners + down[s].astype(jnp.int32)

        @pl.when(up[s])
        def _():
            pl.semaphore_signal(
                barrier, inc=1, device_id=device(OFFSET_LIST[s], 1), device_id_type=pl.DeviceIdType.MESH
            )

    @pl.when(partners > 0)
    def _():
        pl.semaphore_wait(barrier, partners)

    def rows(part):
        return pl.ds(part * half, half)

    def remote(src, dst, send, recv, offset, sign):
        return pltpu.make_async_remote_copy(
            src_ref=src, dst_ref=dst, send_sem=send, recv_sem=recv,
            device_id=device(offset, sign), device_id_type=pl.DeviceIdType.MESH,
        )

    def value_copy(slot, piece, source, offset):
        return remote(
            source.at[piece], values.at[slot, piece],
            value_send.at[slot, len(sent[slot])], value_recv.at[slot, len(sent[slot])], offset, -1,
        )

    sent = {s: [] for s in range(count)}

    def plan(slot, part, source, offset, flag, cuts=(1,)):
        first = part * half
        for cut in cuts:
            piece = pl.ds(first, half // cut)
            sent[slot].append((value_copy(slot, piece, source, offset), piece, flag, part))
            first += half // cut

    for s in (X, Y, Z):
        for part in (0, 1):
            plan(s, part, vectors_ref, OFFSET_LIST[s], down[s])
    plan(XY, 0, values.at[X], OFFSET_LIST[Y], jnp.logical_and(has_up[0], has_down[1]), (2, 2))
    plan(XY, 1, values.at[Y], OFFSET_LIST[X], jnp.logical_and(has_up[1], has_down[0]), (2, 4, 4))
    for part in (0, 1):
        plan(XZ, part, values.at[X], OFFSET_LIST[Z], jnp.logical_and(has_up[0], has_down[2]))

    last = sent[XY][-1]

    def start(slot, part):
        for copy, _, flag, its in sent[slot]:
            if its == part and copy is not last[0]:
                pl.when(flag)(copy.start)

    def arrived(slot, n):
        pl.when(up[slot])(sent[slot][n][0].wait_recv)

    relays = [
        remote(left_out.at[XY, part], relay.at[part], relay_send.at[part], relay_recv.at[part], OFFSET_LIST[s], 1)
        for part, s in ((0, X), (1, Y))
    ]
    onward = [
        remote(relay.at[part], left_in.at[XY, part], left_send.at[XY, part], left_recv.at[XY, part], OFFSET_LIST[s], 1)
        for part, s in ((0, Y), (1, X))
    ]
    passed = (
        ((relays[0], onward[0]), jnp.logical_and(has_down[0], has_up[1])),
        ((relays[1], onward[1]), jnp.logical_and(has_down[1], has_up[0])),
    )
    left_copies = [
        relays if s == XY else [
            remote(left_out.at[s], left_in.at[s], left_send.at[s, 0], left_recv.at[s, 0], OFFSET_LIST[s], 1)
        ]
        for s in range(count)
    ]
    back_copies = [
        remote(back_out.at[s], projected_ref.at[s], back_send.at[s], back_recv.at[s], OFFSET_LIST[s], -1)
        for s in range(count)
    ]

    start(X, 0)
    start(Y, 1)
    start(Z, 0)
    start(X, 1)
    start(Y, 0)
    start(Z, 1)

    for s in LEFT_SLOTS:
        @pl.when(down[s])
        def _():
            pl.semaphore_signal(
                ready.at[s], inc=1, device_id=device(OFFSET_LIST[s], -1), device_id_type=pl.DeviceIdType.MESH
            )

    block_copies = [
        pltpu.make_async_copy(couplings_ref.at[s], blocks.at[s], block_sem.at[s]) for s in range(count)
    ]
    for s in LEFT_ORDER:
        block_copies[s].start()

    basis_copy.wait()
    columns = lax.broadcasted_iota(jnp.int32, (m, k), 1)
    masked = jnp.where(columns < ranks_ref[0, 0, 0], basis[...], 0.0)
    high, low = split2(masked)
    basis_parts[:, :k] = high
    basis_parts[:, k:] = low
    high, low = split2(masked.T)
    stacked[:k] = high
    stacked[k:] = low

    for s in LEFT_SLOTS:
        @pl.when(up[s])
        def _():
            pl.semaphore_wait(ready.at[s], 1)

    for s in LEFT_ORDER:
        block_copies[s].wait()

        @pl.when(up[s])
        def _():
            @pl.loop(0, 2)
            def _(part):
                there = pl.ds(pl.multiple_of(part * half, half), half)
                both = dot32(stacked[...], blocks[s, :, there])
                left_out[s, part] = both[:k] + both[k:]

            if s != XZ:
                for copy in left_copies[s]:
                    copy.start()

    applied_ref[...] = jnp.zeros_like(applied_ref)
    for s in range(count):

        @pl.when(jnp.logical_not(up[s]))
        def _():
            projected_ref[s] = jnp.zeros((k, k), jnp.float32)

    for copy, flag in passed:
        @pl.when(flag)
        def _():
            copy[0].wait_recv()
            copy[1].start()

    pl.when(up[XZ])(left_copies[XZ][0].start)

    tall = min(512, m)

    def apply(slot, n, more=None):
        piece = sent[slot][n][1]
        if more is not None:
            piece = pl.ds(piece.start, piece.size + sent[slot][more][1].size)

        @pl.when(up[slot])
        def _():
            high, low = split2(values[slot, piece])
            pair = jnp.concatenate([high, low], axis=1)

            @pl.loop(0, m // tall)
            def _(step):
                there = pl.ds(pl.multiple_of(step * tall, tall), tall)
                both = dot32(blocks[slot, there, piece], pair)
                applied_ref[there] += both[:, :r] + both[:, r:]

    def project(slot):
        @pl.when(down[slot])
        def _():
            for copy in onward if slot == XY else left_copies[slot]:
                copy.wait_recv()
            out = None
            for part in (0, 1):
                high, low = split2(left_in[slot, part])
                first = dot32(high, basis_parts[rows(part)])
                term = first[:, :k] + first[:, k:] + dot32(low, basis_parts[rows(part), :k])
                out = term if out is None else out + term
            back_out[slot] = out
            back_copies[slot].start()

    even = place[2] % 2 == 0

    def finish(slot, n, more=None):
        arrived(slot, n)
        if more is not None:
            arrived(slot, more)
        apply(slot, n, more)

    arrived(Z, 0)
    apply(Z, 0)
    arrived(X, 0)
    start(XY, 0)
    start(XZ, 0)
    arrived(Y, 1)
    start(XY, 1)
    late = jnp.logical_and(down[XZ], place[2] % 2 == 0)
    pl.when(jnp.logical_and(last[2], jnp.logical_not(late)))(last[0].start)
    arrived(Z, 1)
    apply(Z, 1)
    apply(X, 0)
    apply(Y, 1)
    project(Z)
    project(Y)
    pl.when(even)(lambda: finish(XZ, 0))
    project(X)
    arrived(X, 1)
    start(XZ, 1)
    arrived(Y, 0)
    apply(X, 1)
    apply(Y, 0)
    project(XY)
    pl.when(jnp.logical_not(even))(lambda: finish(XZ, 0))
    pl.when(even)(lambda: finish(XZ, 1))
    project(XZ)
    pl.when(jnp.logical_and(last[2], late))(last[0].start)
    finish(XY, 0)
    finish(XY, 2)
    pl.when(jnp.logical_not(even))(lambda: finish(XZ, 1))
    finish(XY, 1)
    finish(XY, 3, 4)
    for s in range(count):
        pl.when(up[s])(back_copies[s].wait_recv)
    for s in range(count):
        for copy, _, flag, _ in sent[s]:
            pl.when(flag)(copy.wait_send)
        for copy in left_copies[s]:
            pl.when(up[s])(copy.wait_send)
        pl.when(down[s])(back_copies[s].wait_send)
    for copy, flag in passed:
        pl.when(flag)(copy[1].wait_send)


def writer(projected_ref, applied_ref, projected_out, applied_out, sems):
    copies = [
        pltpu.make_async_copy(projected_ref, projected_out, sems.at[0]),
        pltpu.make_async_copy(applied_ref, applied_out, sems.at[1]),
    ]
    for copy in copies:
        copy.start()
    for copy in copies:
        copy.wait()


def solution(mesh):
    sizes = tuple(mesh.shape[name] for name in AXES)

    def local(bases, ranks, couplings, vectors):
        m, k = bases.shape[-2:]
        count = couplings.shape[3]
        r = vectors.shape[-1]
        f32, bf16 = jnp.float32, jnp.bfloat16
        dma = pltpu.SemaphoreType.DMA
        projected, applied = pl.pallas_call(
            functools.partial(kernel, sizes),
            out_shape=(
                pltpu.VMEM((count, k, k), f32),
                pltpu.VMEM((m, r), f32),
            ),
            in_specs=[pl.BlockSpec(memory_space=pltpu.SMEM)] + [pl.BlockSpec(memory_space=pltpu.HBM)] * 3,
            out_specs=(pl.BlockSpec(memory_space=pltpu.VMEM),) * 2,
            scratch_shapes=[
                pltpu.VMEM((m, k), f32),
                pltpu.VMEM((2 * k, m), bf16),
                pltpu.VMEM((m, 2 * k), bf16),
                pltpu.VMEM((count, m, m), bf16),
                pltpu.VMEM((count, m, r), f32),
                pltpu.VMEM((count, 2, k, m // 2), f32),
                pltpu.VMEM((count, 2, k, m // 2), f32),
                pltpu.VMEM((2, k, m // 2), f32),
                pltpu.VMEM((count, k, k), f32),
                pltpu.SemaphoreType.REGULAR((count,)),
                dma,
                dma((count,)),
                dma((count, 5)),
                dma((count, 5)),
                dma((count, 2)),
                dma((count, 2)),
                dma((2,)),
                dma((2,)),
                dma((count,)),
                dma((count,)),
            ],
            compiler_params=pltpu.CompilerParams(collective_id=0, has_side_effects=True, vmem_limit_bytes=64000 << 10),
        )(
            ranks,
            bases.reshape(m, k),
            couplings.reshape(count, m, m),
            vectors.reshape(m, r),
        )
        projected, applied = pl.pallas_call(
            writer,
            out_shape=(jax.ShapeDtypeStruct(projected.shape, f32), jax.ShapeDtypeStruct(applied.shape, f32)),
            in_specs=[pl.BlockSpec(memory_space=pltpu.VMEM)] * 2,
            out_specs=(pl.BlockSpec(memory_space=pltpu.HBM),) * 2,
            scratch_shapes=[dma((2,))],
            compiler_params=pltpu.CompilerParams(vmem_limit_bytes=8 << 20),
        )(projected, applied)
        return (
            projected.reshape(1, 1, 1, count, k, k),
            applied.reshape(1, 1, 1, m, r),
        )

    return jax.shard_map(
        local,
        mesh=mesh,
        in_specs=(
            P("gx", "gy", "gz", None, None),
            P("gx", "gy", "gz"),
            P("gx", "gy", "gz", None, None, None),
            P("gx", "gy", "gz", None, None),
        ),
        out_specs=(P("gx", "gy", "gz", None, None, None), P("gx", "gy", "gz", None, None)),
        check_vma=False,
    )
```

```python
import functools

import jax
import jax.numpy as jnp
from jax import lax
from jax.experimental import pallas as pl
from jax.experimental.pallas import tpu as pltpu
from jax.sharding import PartitionSpec as P

OFFSET_LIST = ((1, 0, 0), (0, 1, 0), (0, 0, 1), (1, 1, 0), (1, 0, 1), (0, 1, 1), (1, 1, 1))
AXES = ("gx", "gy", "gz")
X, Y, Z, XY, XZ = range(5)
LEFT_ORDER = (XY, Y, X, XZ, Z)
LEFT_SLOTS = (X, Y, Z, XZ)


def split2(value):
    high = value.astype(jnp.bfloat16)
    low = (value - high.astype(jnp.float32)).astype(jnp.bfloat16)
    return high, low


def dot32(left, right):
    return jnp.dot(left, right, preferred_element_type=jnp.float32)


def kernel(sizes, *refs):
    dma = pltpu.SemaphoreType.DMA
    count = refs[2].shape[0]
    pl.run_scoped(
        functools.partial(body, sizes, *refs),
        pltpu.SemaphoreType.REGULAR, dma, dma((count,)), dma((12,)), dma((12,)), dma((count + 1,)), dma((count + 1,)),
        dma((2,)), dma((2,)), dma((count,)), dma((count,)),
    )


def body(
    sizes, ranks_ref, bases_ref, couplings_ref, vectors_ref, projected_ref, applied_ref,
    basis, stacked, basis_parts, blocks, values, left_out, left_in, relay, back_out,
    ready, basis_sem, block_sem, value_send, value_recv, left_send, left_recv, relay_send, relay_recv,
    back_send, back_recv,
):
    count, m, k = blocks.shape[0], basis.shape[0], basis.shape[1]
    r = applied_ref.shape[1]
    half = m // 2
    place = [lax.axis_index(name) for name in AXES]
    has_up = [p < n - 1 for p, n in zip(place, sizes)]
    has_down = [p > 0 for p in place]

    def every(flags, offset):
        out = None
        for flag, o in zip(flags, offset):
            if o:
                out = flag if out is None else jnp.logical_and(out, flag)
        return out

    up = [every(has_up, o) for o in OFFSET_LIST[:count]]
    down = [every(has_down, o) for o in OFFSET_LIST[:count]]

    def device(offset, sign):
        return {name: p + sign * o for name, p, o in zip(AXES, place, offset)}

    basis_copy = pltpu.make_async_copy(bases_ref, basis, basis_sem)
    basis_copy.start()

    barrier = pltpu.get_barrier_semaphore()
    partners = jnp.int32(0)
    senders = sum(up[s].astype(jnp.int32) for s in LEFT_SLOTS)
    for s in range(count):
        partners = partners + down[s].astype(jnp.int32)

        @pl.when(up[s])
        def _():
            pl.semaphore_signal(
                barrier, inc=1, device_id=device(OFFSET_LIST[s], 1), device_id_type=pl.DeviceIdType.MESH
            )

    @pl.when(partners > 0)
    def _():
        pl.semaphore_wait(barrier, partners)

    def rows(part):
        return pl.ds(part * half, half)

    def remote(src, dst, send, recv, offset, sign):
        return pltpu.make_async_remote_copy(
            src_ref=src, dst_ref=dst, send_sem=send, recv_sem=recv,
            device_id=device(offset, sign), device_id_type=pl.DeviceIdType.MESH,
        )

    def value_copy(slot, piece, source, offset):
        n = sum(len(copies) for copies in sent.values())
        return remote(
            source.at[piece], values.at[slot, piece], value_send.at[n], value_recv.at[n], offset, -1,
        )

    sent = {s: [] for s in range(count)}

    def plan(slot, part, source, offset, flag, cuts=(4,)):
        first = part * half
        for cut in cuts:
            piece = pl.ds(first, half * cut // 4)
            sent[slot].append((value_copy(slot, piece, source, offset), piece, flag, part))
            first += half * cut // 4

    for s in (X, Y):
        for part in (0, 1):
            plan(s, part, vectors_ref, OFFSET_LIST[s], down[s])
    plan(Z, 0, vectors_ref, OFFSET_LIST[Z], down[Z], (8,))
    plan(XY, 0, values.at[X], OFFSET_LIST[Y], jnp.logical_and(has_up[0], has_down[1]), (2, 2))
    plan(XY, 1, values.at[Y], OFFSET_LIST[X], jnp.logical_and(has_up[1], has_down[0]), (2, 1, 1))
    for part in (0, 1):
        plan(XZ, part, values.at[X], OFFSET_LIST[Z], jnp.logical_and(has_up[0], has_down[2]))

    last = sent[XY][-1]

    def start(slot, part):
        for copy, _, flag, its in sent[slot]:
            if its == part and copy is not last[0]:
                pl.when(flag)(copy.start)

    def arrived(slot, n):
        pl.when(up[slot])(sent[slot][n][0].wait_recv)

    relays = [
        remote(left_out.at[XY, part], relay.at[part], left_send.at[XY + 2 * part], relay_recv.at[part], OFFSET_LIST[s], 1)
        for part, s in ((0, X), (1, Y))
    ]
    onward = [
        remote(relay.at[part], left_in.at[XY, part], relay_send.at[part], left_recv.at[XY + 2 * part], OFFSET_LIST[s], 1)
        for part, s in ((0, Y), (1, X))
    ]
    passed = (
        ((relays[0], onward[0]), jnp.logical_and(has_down[0], has_up[1])),
        ((relays[1], onward[1]), jnp.logical_and(has_down[1], has_up[0])),
    )
    left_copies = [
        relays if s == XY else [
            remote(left_out.at[s], left_in.at[s], left_send.at[s], left_recv.at[s], OFFSET_LIST[s], 1)
        ]
        for s in range(count)
    ]
    back_copies = [
        remote(back_out.at[s], projected_ref.at[s], back_send.at[s], back_recv.at[s], OFFSET_LIST[s], -1)
        for s in range(count)
    ]

    start(X, 0)
    start(Y, 1)
    start(Z, 0)
    start(X, 1)
    start(Y, 0)

    for s in LEFT_SLOTS:
        @pl.when(down[s])
        def _():
            pl.semaphore_signal(
                ready, inc=1, device_id=device(OFFSET_LIST[s], -1), device_id_type=pl.DeviceIdType.MESH
            )

    block_copies = [
        pltpu.make_async_copy(couplings_ref.at[s], blocks.at[s], block_sem.at[s]) for s in range(count)
    ]
    for s in LEFT_ORDER:
        block_copies[s].start()

    basis_copy.wait()
    columns = lax.broadcasted_iota(jnp.int32, (m, k), 1)
    masked = jnp.where(columns < ranks_ref[0, 0, 0], basis[...], 0.0)
    high, low = split2(masked)
    basis_parts[:, :k] = high
    basis_parts[:, k:] = low
    high, low = split2(masked.T)
    stacked[:k] = high
    stacked[k:] = low

    @pl.when(senders > 0)
    def _():
        pl.semaphore_wait(ready, senders)

    for s in LEFT_ORDER:
        block_copies[s].wait()

        @pl.when(up[s])
        def _():
            @pl.loop(0, 2)
            def _(part):
                there = pl.ds(pl.multiple_of(part * half, half), half)
                both = dot32(stacked[...], blocks[s, :, there])
                left_out[s, part] = both[:k] + both[k:]

            if s != XZ:
                for copy in left_copies[s]:
                    copy.start()

    applied_ref[...] = jnp.zeros_like(applied_ref)
    for s in range(count):

        @pl.when(jnp.logical_not(up[s]))
        def _():
            projected_ref[s] = jnp.zeros((k, k), jnp.float32)

    for copy, flag in passed:
        @pl.when(flag)
        def _():
            copy[0].wait_recv()
            copy[1].start()

    pl.when(up[XZ])(left_copies[XZ][0].start)

    tall = min(512, m)

    def apply(slot, n, more=None):
        piece = sent[slot][n][1]
        if more is not None:
            piece = pl.ds(piece.start, piece.size + sent[slot][more][1].size)

        @pl.when(up[slot])
        def _():
            high, low = split2(values[slot, piece])
            pair = jnp.concatenate([high, low], axis=1)

            @pl.loop(0, m // tall)
            def _(step):
                there = pl.ds(pl.multiple_of(step * tall, tall), tall)
                both = dot32(blocks[slot, there, piece], pair)
                applied_ref[there] += both[:, :r] + both[:, r:]

    def project(slot):
        @pl.when(down[slot])
        def _():
            for copy in onward if slot == XY else left_copies[slot]:
                copy.wait_recv()
            out = None
            for part in (0, 1):
                high, low = split2(left_in[slot, part])
                first = dot32(high, basis_parts[rows(part)])
                term = first[:, :k] + first[:, k:] + dot32(low, basis_parts[rows(part), :k])
                out = term if out is None else out + term
            back_out[slot] = out
            back_copies[slot].start()

    even = place[2] % 2 == 0

    def finish(slot, n, more=None):
        arrived(slot, n)
        if more is not None:
            arrived(slot, more)
        apply(slot, n, more)

    arrived(Z, 0)
    apply(Z, 0)
    arrived(X, 0)
    start(XY, 0)
    start(XZ, 0)
    arrived(Y, 1)
    start(XY, 1)
    late = jnp.logical_and(down[XZ], place[2] % 2 == 0)
    pl.when(jnp.logical_and(last[2], jnp.logical_not(late)))(last[0].start)
    apply(X, 0)
    apply(Y, 1)
    project(Z)
    project(Y)
    pl.when(even)(lambda: finish(XZ, 0))
    project(X)
    arrived(X, 1)
    start(XZ, 1)
    arrived(Y, 0)
    apply(X, 1)
    apply(Y, 0)
    project(XY)
    pl.when(jnp.logical_not(even))(lambda: finish(XZ, 0))
    pl.when(even)(lambda: finish(XZ, 1))
    project(XZ)
    pl.when(jnp.logical_and(last[2], late))(last[0].start)
    finish(XY, 0)
    finish(XY, 2)
    pl.when(jnp.logical_not(even))(lambda: finish(XZ, 1))
    finish(XY, 1)
    finish(XY, 3, 4)
    for s in range(count):
        pl.when(up[s])(back_copies[s].wait_recv)
    for s in range(count):
        for copy, _, flag, _ in sent[s]:
            pl.when(flag)(copy.wait_send)
        for copy in left_copies[s]:
            pl.when(up[s])(copy.wait_send)
        pl.when(down[s])(back_copies[s].wait_send)
    for copy, flag in passed:
        pl.when(flag)(copy[1].wait_send)


def writer(*refs):
    pl.run_scoped(functools.partial(write, *refs), pltpu.SemaphoreType.DMA((2,)))


def write(projected_ref, applied_ref, projected_out, applied_out, sems):
    copies = [
        pltpu.make_async_copy(projected_ref, projected_out, sems.at[0]),
        pltpu.make_async_copy(applied_ref, applied_out, sems.at[1]),
    ]
    for copy in copies:
        copy.start()
    for copy in copies:
        copy.wait()


def solution(mesh):
    sizes = tuple(mesh.shape[name] for name in AXES)

    def local(bases, ranks, couplings, vectors):
        m, k = bases.shape[-2:]
        count = couplings.shape[3]
        r = vectors.shape[-1]
        f32, bf16 = jnp.float32, jnp.bfloat16
        projected, applied = pl.pallas_call(
            functools.partial(kernel, sizes),
            out_shape=(
                pltpu.VMEM((count, k, k), f32),
                pltpu.VMEM((m, r), f32),
            ),
            in_specs=[pl.BlockSpec(memory_space=pltpu.SMEM)] + [pl.BlockSpec(memory_space=pltpu.HBM)] * 3,
            out_specs=(pl.BlockSpec(memory_space=pltpu.VMEM),) * 2,
            scratch_shapes=[
                pltpu.VMEM((m, k), f32),
                pltpu.VMEM((2 * k, m), bf16),
                pltpu.VMEM((m, 2 * k), bf16),
                pltpu.VMEM((count, m, m), bf16),
                pltpu.VMEM((count, m, r), f32),
                pltpu.VMEM((count, 2, k, m // 2), f32),
                pltpu.VMEM((count, 2, k, m // 2), f32),
                pltpu.VMEM((2, k, m // 2), f32),
                pltpu.VMEM((count, k, k), f32),
            ],
            compiler_params=pltpu.CompilerParams(collective_id=0, has_side_effects=True, vmem_limit_bytes=64000 << 10),
        )(
            ranks,
            bases.reshape(m, k),
            couplings.reshape(count, m, m),
            vectors.reshape(m, r),
        )
        projected, applied = pl.pallas_call(
            writer,
            out_shape=(jax.ShapeDtypeStruct(projected.shape, f32), jax.ShapeDtypeStruct(applied.shape, f32)),
            in_specs=[pl.BlockSpec(memory_space=pltpu.VMEM)] * 2,
            out_specs=(pl.BlockSpec(memory_space=pltpu.HBM),) * 2,
            compiler_params=pltpu.CompilerParams(vmem_limit_bytes=8 << 20),
        )(projected, applied)
        return (
            projected.reshape(1, 1, 1, count, k, k),
            applied.reshape(1, 1, 1, m, r),
        )

    return jax.shard_map(
        local,
        mesh=mesh,
        in_specs=(
            P("gx", "gy", "gz", None, None),
            P("gx", "gy", "gz"),
            P("gx", "gy", "gz", None, None, None),
            P("gx", "gy", "gz", None, None),
        ),
        out_specs=(P("gx", "gy", "gz", None, None, None), P("gx", "gy", "gz", None, None)),
        check_vma=False,
    )
```

```python
import functools

import jax
import jax.numpy as jnp
from jax import lax
from jax.experimental import pallas as pl
from jax.experimental.pallas import tpu as pltpu
from jax.sharding import PartitionSpec as P

OFFSET_LIST = ((1, 0, 0), (0, 1, 0), (0, 0, 1), (1, 1, 0), (1, 0, 1), (0, 1, 1), (1, 1, 1))
AXES = ("gx", "gy", "gz")
X, Y, Z, XY, XZ = range(5)
LEFT_ORDER = (XY, Y, X, XZ, Z)
LEFT_SLOTS = (X, Y, Z, XZ)


def split2(value):
    high = value.astype(jnp.bfloat16)
    low = (value - high.astype(jnp.float32)).astype(jnp.bfloat16)
    return high, low


def dot32(left, right):
    return jnp.dot(left, right, preferred_element_type=jnp.float32)


def kernel(sizes, *refs):
    dma = pltpu.SemaphoreType.DMA
    count = refs[2].shape[0]
    pl.run_scoped(
        functools.partial(body, sizes, *refs),
        pltpu.SemaphoreType.REGULAR, dma, dma((count,)), dma((12,)), dma((12,)), dma((count + 1,)), dma((count + 1,)),
        dma((2,)), dma((2,)), dma((count,)), dma((count,)),
    )


def body(
    sizes, ranks_ref, bases_ref, couplings_ref, vectors_ref, projected_ref, applied_ref,
    basis, stacked, basis_parts, blocks, values, left_out, left_in, relay, back_out,
    ready, basis_sem, block_sem, value_send, value_recv, left_send, left_recv, relay_send, relay_recv,
    back_send, back_recv,
):
    count, m, k = blocks.shape[0], basis.shape[0], basis.shape[1]
    r = applied_ref.shape[1]
    half = m // 2
    place = [lax.axis_index(name) for name in AXES]
    has_up = [p < n - 1 for p, n in zip(place, sizes)]
    has_down = [p > 0 for p in place]

    def every(flags, offset):
        out = None
        for flag, o in zip(flags, offset):
            if o:
                out = flag if out is None else jnp.logical_and(out, flag)
        return out

    up = [every(has_up, o) for o in OFFSET_LIST[:count]]
    down = [every(has_down, o) for o in OFFSET_LIST[:count]]

    def device(offset, sign):
        return {name: p + sign * o for name, p, o in zip(AXES, place, offset)}

    basis_copy = pltpu.make_async_copy(bases_ref, basis, basis_sem)
    basis_copy.start()

    barrier = pltpu.get_barrier_semaphore()
    partners = jnp.int32(0)
    senders = sum(up[s].astype(jnp.int32) for s in LEFT_SLOTS)
    for s in range(count):
        partners = partners + down[s].astype(jnp.int32)

        @pl.when(up[s])
        def _():
            pl.semaphore_signal(
                barrier, inc=1, device_id=device(OFFSET_LIST[s], 1), device_id_type=pl.DeviceIdType.MESH
            )

    @pl.when(partners > 0)
    def _():
        pl.semaphore_wait(barrier, partners)

    def rows(part):
        return pl.ds(part * half, half)

    def remote(src, dst, send, recv, offset, sign):
        return pltpu.make_async_remote_copy(
            src_ref=src, dst_ref=dst, send_sem=send, recv_sem=recv,
            device_id=device(offset, sign), device_id_type=pl.DeviceIdType.MESH,
        )

    def value_copy(slot, piece, source, offset):
        n = sum(len(copies) for copies in sent.values())
        return remote(
            source.at[piece], values.at[slot, piece], value_send.at[n], value_recv.at[n], offset, -1,
        )

    sent = {s: [] for s in range(count)}
    quarter, eighth, shift = m // 4, m // 16, m // 64

    def plan(slot, part, source, offset, flag, *cuts):
        for first, size in cuts:
            piece = pl.ds(first, size)
            sent[slot].append((value_copy(slot, piece, source, offset), piece, flag, part))

    for part in (0, 1):
        plan(X, part, vectors_ref, OFFSET_LIST[X], down[X], (part * half, half))
    plan(Y, 0, vectors_ref, OFFSET_LIST[Y], down[Y], (0, half - shift))
    plan(Y, 1, vectors_ref, OFFSET_LIST[Y], down[Y], (half - shift, half + shift))
    plan(Z, 0, vectors_ref, OFFSET_LIST[Z], down[Z], (0, m))
    plan(
        XY, 0, values.at[X], OFFSET_LIST[Y], jnp.logical_and(has_up[0], has_down[1]),
        (0, quarter), (quarter, quarter - shift),
    )
    by_y = jnp.logical_and(has_up[1], has_down[0])
    plan(XY, 1, values.at[Y], OFFSET_LIST[X], by_y, (half - shift, quarter + shift), (half + quarter, quarter - eighth))
    plan(XY, 2, values.at[Y], OFFSET_LIST[X], by_y, (m - eighth, eighth))
    for part in (0, 1):
        plan(
            XZ, part, values.at[X], OFFSET_LIST[Z], jnp.logical_and(has_up[0], has_down[2]), (part * half, half),
        )

    def start(slot, part):
        for copy, _, flag, its in sent[slot]:
            if its == part:
                pl.when(flag)(copy.start)

    def arrived(slot, n):
        pl.when(up[slot])(sent[slot][n][0].wait_recv)

    relays = [
        remote(left_out.at[XY, part], relay.at[part], left_send.at[XY + 2 * part], relay_recv.at[part], OFFSET_LIST[s], 1)
        for part, s in ((0, X), (1, Y))
    ]
    onward = [
        remote(relay.at[part], left_in.at[XY, part], relay_send.at[part], left_recv.at[XY + 2 * part], OFFSET_LIST[s], 1)
        for part, s in ((0, Y), (1, X))
    ]
    passed = (
        ((relays[0], onward[0]), jnp.logical_and(has_down[0], has_up[1])),
        ((relays[1], onward[1]), jnp.logical_and(has_down[1], has_up[0])),
    )
    left_copies = [
        relays if s == XY else [
            remote(left_out.at[s], left_in.at[s], left_send.at[s], left_recv.at[s], OFFSET_LIST[s], 1)
        ]
        for s in range(count)
    ]
    back_copies = [
        remote(back_out.at[s], projected_ref.at[s], back_send.at[s], back_recv.at[s], OFFSET_LIST[s], -1)
        for s in range(count)
    ]

    start(X, 0)
    start(Y, 1)
    start(Z, 0)
    start(X, 1)
    start(Y, 0)

    for s in LEFT_SLOTS:
        @pl.when(down[s])
        def _():
            pl.semaphore_signal(
                ready, inc=1, device_id=device(OFFSET_LIST[s], -1), device_id_type=pl.DeviceIdType.MESH
            )

    block_copies = [
        pltpu.make_async_copy(couplings_ref.at[s], blocks.at[s], block_sem.at[s]) for s in range(count)
    ]
    for s in LEFT_ORDER:
        block_copies[s].start()

    basis_copy.wait()
    columns = lax.broadcasted_iota(jnp.int32, (m, k), 1)
    masked = jnp.where(columns < ranks_ref[0, 0, 0], basis[...], 0.0)
    high, low = split2(masked)
    basis_parts[:, :k] = high
    basis_parts[:, k:] = low
    high, low = split2(masked.T)
    stacked[:k] = high
    stacked[k:] = low

    @pl.when(senders > 0)
    def _():
        pl.semaphore_wait(ready, senders)

    for s in LEFT_ORDER:
        block_copies[s].wait()

        @pl.when(up[s])
        def _():
            @pl.loop(0, 2)
            def _(part):
                there = pl.ds(pl.multiple_of(part * half, half), half)
                both = dot32(stacked[...], blocks[s, :, there])
                left_out[s, part] = both[:k] + both[k:]

            if s != XZ:
                for copy in left_copies[s]:
                    copy.start()

    applied_ref[...] = jnp.zeros_like(applied_ref)
    for s in range(count):

        @pl.when(jnp.logical_not(up[s]))
        def _():
            projected_ref[s] = jnp.zeros((k, k), jnp.float32)

    for copy, flag in passed:
        @pl.when(flag)
        def _():
            copy[0].wait_recv()
            copy[1].start()

    pl.when(up[XZ])(left_copies[XZ][0].start)

    tall = min(512, m)

    def apply(slot, piece):
        @pl.when(up[slot])
        def _():
            high, low = split2(values[slot, piece])
            pair = jnp.concatenate([high, low], axis=1)

            @pl.loop(0, m // tall)
            def _(step):
                there = pl.ds(pl.multiple_of(step * tall, tall), tall)
                both = dot32(blocks[slot, there, piece], pair)
                applied_ref[there] += both[:, :r] + both[:, r:]

    def project(slot):
        @pl.when(down[slot])
        def _():
            for copy in onward if slot == XY else left_copies[slot]:
                copy.wait_recv()
            out = None
            for part in (0, 1):
                high, low = split2(left_in[slot, part])
                first = dot32(high, basis_parts[rows(part)])
                term = first[:, :k] + first[:, k:] + dot32(low, basis_parts[rows(part), :k])
                out = term if out is None else out + term
            back_out[slot] = out
            if slot == X:
                pl.when(jnp.logical_not(late))(back_copies[slot].start)
            else:
                back_copies[slot].start()

    even = place[2] % 2 == 0
    late = down[XZ]

    def finish(slot, first, size, *pieces):
        for n in pieces:
            arrived(slot, n)
        apply(slot, pl.ds(first, size))

    finish(Z, 0, m, 0)
    arrived(X, 0)
    start(XY, 0)
    start(XZ, 0)
    arrived(Y, 1)
    start(XY, 1)
    pl.when(jnp.logical_not(late))(lambda: start(XY, 2))
    apply(X, pl.ds(0, half))
    apply(Y, pl.ds(half, half))
    project(Z)
    project(Y)
    pl.when(even)(lambda: finish(XZ, 0, half, 0))
    project(X)
    arrived(X, 1)
    start(XZ, 1)
    arrived(Y, 0)
    apply(X, pl.ds(half, half))
    apply(Y, pl.ds(0, half))
    project(XY)
    pl.when(jnp.logical_not(even))(lambda: finish(XZ, 0, half, 0))
    pl.when(even)(lambda: finish(XZ, half, half, 1))
    project(XZ)
    pl.when(late)(lambda: start(XY, 2))
    pl.when(jnp.logical_and(late, down[X]))(back_copies[X].start)
    finish(XY, 0, quarter, 0)
    finish(XY, half, quarter, 2)
    pl.when(jnp.logical_not(even))(lambda: finish(XZ, half, half, 1))
    held = place[2] > 0
    pl.when(jnp.logical_not(held))(lambda: finish(XY, half + quarter, quarter, 3, 4))
    finish(XY, quarter, quarter, 1)
    pl.when(held)(lambda: finish(XY, half + quarter, quarter, 3, 4))
    for s in range(count):
        pl.when(up[s])(back_copies[s].wait_recv)
    for s in range(count):
        for copy, _, flag, _ in sent[s]:
            pl.when(flag)(copy.wait_send)
        for copy in left_copies[s]:
            pl.when(up[s])(copy.wait_send)
        pl.when(down[s])(back_copies[s].wait_send)
    for copy, flag in passed:
        pl.when(flag)(copy[1].wait_send)


def writer(*refs):
    pl.run_scoped(functools.partial(write, *refs), pltpu.SemaphoreType.DMA((2,)))


def write(projected_ref, applied_ref, projected_out, applied_out, sems):
    copies = [
        pltpu.make_async_copy(projected_ref, projected_out, sems.at[0]),
        pltpu.make_async_copy(applied_ref, applied_out, sems.at[1]),
    ]
    for copy in copies:
        copy.start()
    for copy in copies:
        copy.wait()


def solution(mesh):
    sizes = tuple(mesh.shape[name] for name in AXES)

    def local(bases, ranks, couplings, vectors):
        m, k = bases.shape[-2:]
        count = couplings.shape[3]
        r = vectors.shape[-1]
        f32, bf16 = jnp.float32, jnp.bfloat16
        projected, applied = pl.pallas_call(
            functools.partial(kernel, sizes),
            out_shape=(
                pltpu.VMEM((count, k, k), f32),
                pltpu.VMEM((m, r), f32),
            ),
            in_specs=[pl.BlockSpec(memory_space=pltpu.SMEM)] + [pl.BlockSpec(memory_space=pltpu.HBM)] * 3,
            out_specs=(pl.BlockSpec(memory_space=pltpu.VMEM),) * 2,
            scratch_shapes=[
                pltpu.VMEM((m, k), f32),
                pltpu.VMEM((2 * k, m), bf16),
                pltpu.VMEM((m, 2 * k), bf16),
                pltpu.VMEM((count, m, m), bf16),
                pltpu.VMEM((count, m, r), f32),
                pltpu.VMEM((count, 2, k, m // 2), f32),
                pltpu.VMEM((count, 2, k, m // 2), f32),
                pltpu.VMEM((2, k, m // 2), f32),
                pltpu.VMEM((count, k, k), f32),
            ],
            compiler_params=pltpu.CompilerParams(collective_id=0, has_side_effects=True, vmem_limit_bytes=64000 << 10),
        )(
            ranks,
            bases.reshape(m, k),
            couplings.reshape(count, m, m),
            vectors.reshape(m, r),
        )
        projected, applied = pl.pallas_call(
            writer,
            out_shape=(jax.ShapeDtypeStruct(projected.shape, f32), jax.ShapeDtypeStruct(applied.shape, f32)),
            in_specs=[pl.BlockSpec(memory_space=pltpu.VMEM)] * 2,
            out_specs=(pl.BlockSpec(memory_space=pltpu.HBM),) * 2,
            compiler_params=pltpu.CompilerParams(vmem_limit_bytes=8 << 20),
        )(projected, applied)
        return (
            projected.reshape(1, 1, 1, count, k, k),
            applied.reshape(1, 1, 1, m, r),
        )

    return jax.shard_map(
        local,
        mesh=mesh,
        in_specs=(
            P("gx", "gy", "gz", None, None),
            P("gx", "gy", "gz"),
            P("gx", "gy", "gz", None, None, None),
            P("gx", "gy", "gz", None, None),
        ),
        out_specs=(P("gx", "gy", "gz", None, None, None), P("gx", "gy", "gz", None, None)),
        check_vma=False,
    )
```

```python
import functools

import jax
import jax.numpy as jnp
from jax import lax
from jax.experimental import pallas as pl
from jax.experimental.pallas import tpu as pltpu
from jax.sharding import PartitionSpec as P

OFFSET_LIST = ((1, 0, 0), (0, 1, 0), (0, 0, 1), (1, 1, 0), (1, 0, 1), (0, 1, 1), (1, 1, 1))
AXES = ("gx", "gy", "gz")
X, Y, Z, XY, XZ = range(5)
LEFT_ORDER = (XY, Y, X, XZ, Z)


def split2(value):
    high = value.astype(jnp.bfloat16)
    low = (value - high.astype(jnp.float32)).astype(jnp.bfloat16)
    return high, low


def dot32(left, right):
    return jnp.dot(left, right, preferred_element_type=jnp.float32)


def kernel(sizes, *refs):
    dma = pltpu.SemaphoreType.DMA
    count = refs[2].shape[0]
    pl.run_scoped(
        functools.partial(body, sizes, *refs),
        pltpu.SemaphoreType.REGULAR, pltpu.SemaphoreType.REGULAR, dma, dma((count,)), dma((12,)), dma((12,)),
        dma((count + 1,)), dma((count + 1,)), dma((2,)), dma((2,)), dma((count,)), dma((count,)),
    )


def body(
    sizes, ranks_ref, bases_ref, couplings_ref, vectors_ref, projected_ref, applied_ref,
    basis, stacked, basis_parts, blocks, values, left_out, left_in, relay, back_out,
    ready, beyond, basis_sem, block_sem, value_send, value_recv, left_send, left_recv, relay_send, relay_recv,
    back_send, back_recv,
):
    count, m, k = blocks.shape[0], basis.shape[0], basis.shape[1]
    r = applied_ref.shape[1]
    half = m // 2
    place = [lax.axis_index(name) for name in AXES]
    has_up = [p < n - 1 for p, n in zip(place, sizes)]
    has_down = [p > 0 for p in place]

    def every(flags, offset):
        out = None
        for flag, o in zip(flags, offset):
            if o:
                out = flag if out is None else jnp.logical_and(out, flag)
        return out

    up = [every(has_up, o) for o in OFFSET_LIST[:count]]
    down = [every(has_down, o) for o in OFFSET_LIST[:count]]

    def device(offset, sign):
        return {name: p + sign * o for name, p, o in zip(AXES, place, offset)}

    basis_copy = pltpu.make_async_copy(bases_ref, basis, basis_sem)
    basis_copy.start()

    even = place[2] % 2 == 0
    odd = jnp.logical_not(even)

    def tell(flag, semaphore, offset, sign):
        @pl.when(flag)
        def _():
            pl.semaphore_signal(
                semaphore, inc=1, device_id=device(offset, sign), device_id_type=pl.DeviceIdType.MESH
            )

    def number(*flags):
        return sum(flag.astype(jnp.int32) for flag in flags)

    def hear(semaphore, amount):
        @pl.when(amount > 0)
        def _():
            pl.semaphore_wait(semaphore, amount)

    barrier = pltpu.get_barrier_semaphore()
    along_x, along_y, along_z = (OFFSET_LIST[s] for s in (X, Y, Z))
    tell(up[X], barrier, along_x, 1)
    tell(up[Y], barrier, along_y, 1)
    tell(jnp.logical_and(odd, up[Z]), barrier, along_z, 1)
    tell(jnp.logical_and(odd, down[Z]), barrier, along_z, -1)
    hear(barrier, number(down[X], down[Y], jnp.logical_and(even, down[Z]), jnp.logical_and(even, up[Z])))

    def rows(part):
        return pl.ds(part * half, half)

    def remote(src, dst, send, recv, offset, sign):
        return pltpu.make_async_remote_copy(
            src_ref=src, dst_ref=dst, send_sem=send, recv_sem=recv,
            device_id=device(offset, sign), device_id_type=pl.DeviceIdType.MESH,
        )

    def value_copy(slot, piece, source, offset):
        n = sum(len(copies) for copies in sent.values())
        return remote(
            source.at[piece], values.at[slot, piece], value_send.at[n], value_recv.at[n], offset, -1,
        )

    sent = {s: [] for s in range(count)}
    quarter, eighth, shift = m // 4, m // 16, m // 64

    def plan(slot, part, source, offset, flag, *cuts):
        for first, size in cuts:
            piece = pl.ds(first, size)
            sent[slot].append((value_copy(slot, piece, source, offset), piece, flag, part))

    for part in (0, 1):
        plan(X, part, vectors_ref, OFFSET_LIST[X], down[X], (part * half, half))
    plan(Y, 0, vectors_ref, OFFSET_LIST[Y], down[Y], (0, half - shift))
    plan(Y, 1, vectors_ref, OFFSET_LIST[Y], down[Y], (half - shift, half + shift))
    plan(Z, 0, vectors_ref, OFFSET_LIST[Z], down[Z], (0, m))
    plan(
        XY, 0, values.at[X], OFFSET_LIST[Y], jnp.logical_and(has_up[0], has_down[1]),
        (0, quarter), (quarter, quarter - shift),
    )
    by_y = jnp.logical_and(has_up[1], has_down[0])
    plan(XY, 1, values.at[Y], OFFSET_LIST[X], by_y, (half - shift, quarter + shift), (half + quarter, quarter - eighth))
    plan(XY, 2, values.at[Y], OFFSET_LIST[X], by_y, (m - eighth, eighth))
    for part in (0, 1):
        plan(
            XZ, part, values.at[X], OFFSET_LIST[Z], jnp.logical_and(has_up[0], has_down[2]), (part * half, half),
        )

    def start(slot, part):
        for copy, _, flag, its in sent[slot]:
            if its == part:
                pl.when(flag)(copy.start)

    def arrived(slot, n):
        pl.when(up[slot])(sent[slot][n][0].wait_recv)

    relays = [
        remote(left_out.at[XY, part], relay.at[part], left_send.at[XY + 2 * part], relay_recv.at[part], OFFSET_LIST[s], 1)
        for part, s in ((0, X), (1, Y))
    ]
    onward = [
        remote(relay.at[part], left_in.at[XY, part], relay_send.at[part], left_recv.at[XY + 2 * part], OFFSET_LIST[s], 1)
        for part, s in ((0, Y), (1, X))
    ]
    passed = (
        ((relays[0], onward[0]), jnp.logical_and(has_down[0], has_up[1])),
        ((relays[1], onward[1]), jnp.logical_and(has_down[1], has_up[0])),
    )
    left_copies = [
        relays if s == XY else [
            remote(left_out.at[s], left_in.at[s], left_send.at[s], left_recv.at[s], OFFSET_LIST[s], 1)
        ]
        for s in range(count)
    ]
    back_copies = [
        remote(back_out.at[s], projected_ref.at[s], back_send.at[s], back_recv.at[s], OFFSET_LIST[s], -1)
        for s in range(count)
    ]

    start(X, 0)
    start(Y, 1)
    pl.when(even)(lambda: start(Z, 0))
    start(X, 1)
    start(Y, 0)
    tell(down[X], ready, along_x, -1)
    tell(down[Y], ready, along_y, -1)
    tell(jnp.logical_and(even, down[Z]), ready, along_z, -1)
    tell(jnp.logical_and(even, up[Z]), ready, along_z, 1)

    block_copies = [
        pltpu.make_async_copy(couplings_ref.at[s], blocks.at[s], block_sem.at[s]) for s in range(count)
    ]
    for s in LEFT_ORDER:
        block_copies[s].start()

    basis_copy.wait()
    columns = lax.broadcasted_iota(jnp.int32, (m, k), 1)
    masked = jnp.where(columns < ranks_ref[0, 0, 0], basis[...], 0.0)
    high, low = split2(masked)
    basis_parts[:, :k] = high
    basis_parts[:, k:] = low
    high, low = split2(masked.T)
    stacked[:k] = high
    stacked[k:] = low

    hear(ready, number(up[X], up[Y], jnp.logical_and(odd, up[Z]), jnp.logical_and(odd, down[Z])))
    tell(jnp.logical_and(down[Z], up[X]), beyond, along_z, -1)
    pl.when(odd)(lambda: start(Z, 0))

    for s in LEFT_ORDER:
        block_copies[s].wait()

        @pl.when(up[s])
        def _():
            @pl.loop(0, 2)
            def _(part):
                there = pl.ds(pl.multiple_of(part * half, half), half)
                both = dot32(stacked[...], blocks[s, :, there])
                left_out[s, part] = both[:k] + both[k:]

            if s != XZ:
                for copy in left_copies[s]:
                    copy.start()

    applied_ref[...] = jnp.zeros_like(applied_ref)
    for s in range(count):

        @pl.when(jnp.logical_not(up[s]))
        def _():
            projected_ref[s] = jnp.zeros((k, k), jnp.float32)

    for copy, flag in passed:
        @pl.when(flag)
        def _():
            copy[0].wait_recv()
            copy[1].start()

    @pl.when(up[XZ])
    def _():
        pl.semaphore_wait(beyond, 1)
        left_copies[XZ][0].start()

    tall = min(512, m)

    def apply(slot, piece):
        @pl.when(up[slot])
        def _():
            high, low = split2(values[slot, piece])
            pair = jnp.concatenate([high, low], axis=1)

            @pl.loop(0, m // tall)
            def _(step):
                there = pl.ds(pl.multiple_of(step * tall, tall), tall)
                both = dot32(blocks[slot, there, piece], pair)
                applied_ref[there] += both[:, :r] + both[:, r:]

    def project(slot):
        @pl.when(down[slot])
        def _():
            for copy in onward if slot == XY else left_copies[slot]:
                copy.wait_recv()
            out = None
            for part in (0, 1):
                high, low = split2(left_in[slot, part])
                first = dot32(high, basis_parts[rows(part)])
                term = first[:, :k] + first[:, k:] + dot32(low, basis_parts[rows(part), :k])
                out = term if out is None else out + term
            back_out[slot] = out
            if slot == X:
                pl.when(jnp.logical_not(late))(back_copies[slot].start)
            else:
                back_copies[slot].start()

    late = down[XZ]

    def finish(slot, first, size, *pieces):
        for n in pieces:
            arrived(slot, n)
        apply(slot, pl.ds(first, size))

    finish(Z, 0, m, 0)
    arrived(X, 0)
    start(XY, 0)
    start(XZ, 0)
    arrived(Y, 1)
    start(XY, 1)
    pl.when(jnp.logical_not(late))(lambda: start(XY, 2))
    apply(X, pl.ds(0, half))
    apply(Y, pl.ds(half, half))
    project(Z)
    project(Y)
    pl.when(even)(lambda: finish(XZ, 0, half, 0))
    project(X)
    arrived(X, 1)
    start(XZ, 1)
    arrived(Y, 0)
    apply(X, pl.ds(half, half))
    apply(Y, pl.ds(0, half))
    project(XY)
    pl.when(odd)(lambda: finish(XZ, 0, half, 0))
    pl.when(even)(lambda: finish(XZ, half, half, 1))
    project(XZ)
    pl.when(late)(lambda: start(XY, 2))
    pl.when(jnp.logical_and(late, down[X]))(back_copies[X].start)
    finish(XY, 0, quarter, 0)
    finish(XY, half, quarter, 2)
    pl.when(odd)(lambda: finish(XZ, half, half, 1))
    held = place[2] > 0
    pl.when(jnp.logical_not(held))(lambda: finish(XY, half + quarter, quarter, 3, 4))
    finish(XY, quarter, quarter, 1)
    pl.when(held)(lambda: finish(XY, half + quarter, quarter, 3, 4))
    for s in range(count):
        pl.when(up[s])(back_copies[s].wait_recv)
    for s in range(count):
        for copy, _, flag, _ in sent[s]:
            pl.when(flag)(copy.wait_send)
        for copy in left_copies[s]:
            pl.when(up[s])(copy.wait_send)
        pl.when(down[s])(back_copies[s].wait_send)
    for copy, flag in passed:
        pl.when(flag)(copy[1].wait_send)


def writer(*refs):
    pl.run_scoped(functools.partial(write, *refs), pltpu.SemaphoreType.DMA((2,)))


def write(projected_ref, applied_ref, projected_out, applied_out, sems):
    copies = [
        pltpu.make_async_copy(projected_ref, projected_out, sems.at[0]),
        pltpu.make_async_copy(applied_ref, applied_out, sems.at[1]),
    ]
    for copy in copies:
        copy.start()
    for copy in copies:
        copy.wait()


def solution(mesh):
    sizes = tuple(mesh.shape[name] for name in AXES)

    def local(bases, ranks, couplings, vectors):
        m, k = bases.shape[-2:]
        count = couplings.shape[3]
        r = vectors.shape[-1]
        f32, bf16 = jnp.float32, jnp.bfloat16
        projected, applied = pl.pallas_call(
            functools.partial(kernel, sizes),
            out_shape=(
                pltpu.VMEM((count, k, k), f32),
                pltpu.VMEM((m, r), f32),
            ),
            in_specs=[pl.BlockSpec(memory_space=pltpu.SMEM)] + [pl.BlockSpec(memory_space=pltpu.HBM)] * 3,
            out_specs=(pl.BlockSpec(memory_space=pltpu.VMEM),) * 2,
            scratch_shapes=[
                pltpu.VMEM((m, k), f32),
                pltpu.VMEM((2 * k, m), bf16),
                pltpu.VMEM((m, 2 * k), bf16),
                pltpu.VMEM((count, m, m), bf16),
                pltpu.VMEM((count, m, r), f32),
                pltpu.VMEM((count, 2, k, m // 2), f32),
                pltpu.VMEM((count, 2, k, m // 2), f32),
                pltpu.VMEM((2, k, m // 2), f32),
                pltpu.VMEM((count, k, k), f32),
            ],
            compiler_params=pltpu.CompilerParams(collective_id=0, has_side_effects=True, vmem_limit_bytes=64000 << 10),
        )(
            ranks,
            bases.reshape(m, k),
            couplings.reshape(count, m, m),
            vectors.reshape(m, r),
        )
        projected, applied = pl.pallas_call(
            writer,
            out_shape=(jax.ShapeDtypeStruct(projected.shape, f32), jax.ShapeDtypeStruct(applied.shape, f32)),
            in_specs=[pl.BlockSpec(memory_space=pltpu.VMEM)] * 2,
            out_specs=(pl.BlockSpec(memory_space=pltpu.HBM),) * 2,
            compiler_params=pltpu.CompilerParams(vmem_limit_bytes=8 << 20),
        )(projected, applied)
        return (
            projected.reshape(1, 1, 1, count, k, k),
            applied.reshape(1, 1, 1, m, r),
        )

    return jax.shard_map(
        local,
        mesh=mesh,
        in_specs=(
            P("gx", "gy", "gz", None, None),
            P("gx", "gy", "gz"),
            P("gx", "gy", "gz", None, None, None),
            P("gx", "gy", "gz", None, None),
        ),
        out_specs=(P("gx", "gy", "gz", None, None, None), P("gx", "gy", "gz", None, None)),
        check_vma=False,
    )
```

```python
import functools

import jax
import jax.numpy as jnp
from jax import lax
from jax.experimental import pallas as pl
from jax.experimental.pallas import tpu as pltpu
from jax.sharding import PartitionSpec as P

OFFSET_LIST = ((1, 0, 0), (0, 1, 0), (0, 0, 1), (1, 1, 0), (1, 0, 1), (0, 1, 1), (1, 1, 1))
AXES = ("gx", "gy", "gz")
X, Y, Z, XY, XZ = range(5)
LEFT_ORDER = (XY, Y, X, XZ, Z)


def split2(value):
    high = value.astype(jnp.bfloat16)
    low = (value - high.astype(jnp.float32)).astype(jnp.bfloat16)
    return high, low


def dot32(left, right):
    return jnp.dot(left, right, preferred_element_type=jnp.float32)


def kernel(sizes, *refs):
    dma = pltpu.SemaphoreType.DMA
    count = refs[2].shape[0]
    pl.run_scoped(
        functools.partial(body, sizes, *refs),
        pltpu.SemaphoreType.REGULAR, pltpu.SemaphoreType.REGULAR, dma, dma((count,)), dma((12,)), dma((12,)),
        dma((count + 1,)), dma((count + 1,)), dma((2,)), dma((2,)), dma((count,)), dma((count,)),
    )


def body(
    sizes, ranks_ref, bases_ref, couplings_ref, vectors_ref, projected_ref, applied_ref,
    basis, stacked, basis_parts, blocks, values, left_out, left_in, relay, back_out,
    ready, beyond, basis_sem, block_sem, value_send, value_recv, left_send, left_recv, relay_send, relay_recv,
    back_send, back_recv,
):
    count, m, k = blocks.shape[0], basis.shape[0], basis.shape[1]
    r = applied_ref.shape[1]
    half = m // 2
    place = [lax.axis_index(name) for name in AXES]
    has_up = [p < n - 1 for p, n in zip(place, sizes)]
    has_down = [p > 0 for p in place]

    def every(flags, offset):
        out = None
        for flag, o in zip(flags, offset):
            if o:
                out = flag if out is None else jnp.logical_and(out, flag)
        return out

    up = [every(has_up, o) for o in OFFSET_LIST[:count]]
    down = [every(has_down, o) for o in OFFSET_LIST[:count]]

    def device(offset, sign):
        return {name: p + sign * o for name, p, o in zip(AXES, place, offset)}

    basis_copy = pltpu.make_async_copy(bases_ref, basis, basis_sem)
    basis_copy.start()

    even = place[2] % 2 == 0
    odd = jnp.logical_not(even)

    def tell(flag, semaphore, offset, sign):
        @pl.when(flag)
        def _():
            pl.semaphore_signal(
                semaphore, inc=1, device_id=device(offset, sign), device_id_type=pl.DeviceIdType.MESH
            )

    def number(*flags):
        return sum(flag.astype(jnp.int32) for flag in flags)

    def hear(semaphore, amount):
        @pl.when(amount > 0)
        def _():
            pl.semaphore_wait(semaphore, amount)

    barrier = pltpu.get_barrier_semaphore()
    along_x, along_y, along_z = (OFFSET_LIST[s] for s in (X, Y, Z))
    tell(up[X], barrier, along_x, 1)
    tell(up[Y], barrier, along_y, 1)
    tell(jnp.logical_and(odd, up[Z]), barrier, along_z, 1)
    tell(jnp.logical_and(odd, down[Z]), barrier, along_z, -1)
    hear(barrier, number(down[X], down[Y], jnp.logical_and(even, down[Z]), jnp.logical_and(even, up[Z])))

    def rows(part):
        return pl.ds(part * half, half)

    def remote(src, dst, send, recv, offset, sign):
        return pltpu.make_async_remote_copy(
            src_ref=src, dst_ref=dst, send_sem=send, recv_sem=recv,
            device_id=device(offset, sign), device_id_type=pl.DeviceIdType.MESH,
        )

    def value_copy(slot, piece, source, offset):
        n = sum(len(copies) for copies in sent.values())
        return remote(
            source.at[piece], values.at[slot, piece], value_send.at[n], value_recv.at[n], offset, -1,
        )

    sent = {s: [] for s in range(count)}
    quarter, eighth, shift = m // 4, m // 16, m // 64

    def plan(slot, part, source, offset, flag, *cuts):
        for first, size in cuts:
            piece = pl.ds(first, size)
            sent[slot].append((value_copy(slot, piece, source, offset), piece, flag, part))

    for part in (0, 1):
        plan(X, part, vectors_ref, OFFSET_LIST[X], down[X], (part * half, half))
    plan(Y, 0, vectors_ref, OFFSET_LIST[Y], down[Y], (0, half - shift))
    plan(Y, 1, vectors_ref, OFFSET_LIST[Y], down[Y], (half - shift, half + shift))
    plan(Z, 0, vectors_ref, OFFSET_LIST[Z], down[Z], (0, m))
    plan(
        XY, 0, values.at[X], OFFSET_LIST[Y], jnp.logical_and(has_up[0], has_down[1]),
        (0, quarter), (quarter, quarter - shift),
    )
    by_y = jnp.logical_and(has_up[1], has_down[0])
    plan(XY, 1, values.at[Y], OFFSET_LIST[X], by_y, (half - shift, quarter + shift), (half + quarter, quarter - eighth))
    plan(XY, 2, values.at[Y], OFFSET_LIST[X], by_y, (m - eighth, eighth))
    for part in (0, 1):
        plan(
            XZ, part, values.at[X], OFFSET_LIST[Z], jnp.logical_and(has_up[0], has_down[2]), (part * half, half),
        )

    def start(slot, part):
        for copy, _, flag, its in sent[slot]:
            if its == part:
                pl.when(flag)(copy.start)

    def arrived(slot, n):
        pl.when(up[slot])(sent[slot][n][0].wait_recv)

    relays = [
        remote(left_out.at[XY, part], relay.at[part], left_send.at[XY + 2 * part], relay_recv.at[part], OFFSET_LIST[s], 1)
        for part, s in ((0, X), (1, Y))
    ]
    onward = [
        remote(relay.at[part], left_in.at[XY, part], relay_send.at[part], left_recv.at[XY + 2 * part], OFFSET_LIST[s], 1)
        for part, s in ((0, Y), (1, X))
    ]
    passed = (
        ((relays[0], onward[0]), jnp.logical_and(has_down[0], has_up[1])),
        ((relays[1], onward[1]), jnp.logical_and(has_down[1], has_up[0])),
    )
    left_copies = [
        relays if s == XY else [
            remote(left_out.at[s], left_in.at[s], left_send.at[s], left_recv.at[s], OFFSET_LIST[s], 1)
        ]
        for s in range(count)
    ]
    back_copies = [
        remote(back_out.at[s], projected_ref.at[s], back_send.at[s], back_recv.at[s], OFFSET_LIST[s], -1)
        for s in range(count)
    ]

    start(X, 0)
    start(Y, 1)
    pl.when(even)(lambda: start(Z, 0))
    start(X, 1)
    start(Y, 0)
    tell(down[X], ready, along_x, -1)
    tell(down[Y], ready, along_y, -1)
    tell(jnp.logical_and(even, down[Z]), ready, along_z, -1)
    tell(jnp.logical_and(even, up[Z]), ready, along_z, 1)

    block_copies = [
        pltpu.make_async_copy(couplings_ref.at[s], blocks.at[s], block_sem.at[s]) for s in range(count)
    ]
    for s in LEFT_ORDER:
        block_copies[s].start()

    basis_copy.wait()
    columns = lax.broadcasted_iota(jnp.int32, (m, k), 1)
    masked = jnp.where(columns < ranks_ref[0, 0, 0], basis[...], 0.0)
    high, low = split2(masked)
    basis_parts[:, :k] = high
    basis_parts[:, k:] = low
    high, low = split2(masked.T)
    stacked[:k] = high
    stacked[k:] = low

    hear(ready, number(up[X], up[Y], jnp.logical_and(odd, up[Z]), jnp.logical_and(odd, down[Z])))
    tell(jnp.logical_and(down[Z], up[X]), beyond, along_z, -1)
    pl.when(odd)(lambda: start(Z, 0))

    for s in LEFT_ORDER:
        block_copies[s].wait()

        @pl.when(up[s])
        def _():
            @pl.loop(0, 2)
            def _(part):
                there = pl.ds(pl.multiple_of(part * half, half), half)
                both = dot32(stacked[...], blocks[s, :, there])
                left_out[s, part] = both[:k] + both[k:]

            if s != XZ:
                for copy in left_copies[s]:
                    copy.start()

    applied_ref[...] = jnp.zeros_like(applied_ref)
    for s in range(count):

        @pl.when(jnp.logical_not(up[s]))
        def _():
            projected_ref[s] = jnp.zeros((k, k), jnp.float32)

    for copy, flag in passed:
        @pl.when(flag)
        def _():
            copy[0].wait_recv()
            copy[1].start()

    @pl.when(up[XZ])
    def _():
        pl.semaphore_wait(beyond, 1)
        left_copies[XZ][0].start()

    tall = min(512, m)

    def apply(slot, piece):
        @pl.when(up[slot])
        def _():
            high, low = split2(values[slot, piece])
            pair = jnp.concatenate([high, low], axis=1)

            @pl.loop(0, m // tall)
            def _(step):
                there = pl.ds(pl.multiple_of(step * tall, tall), tall)
                both = dot32(blocks[slot, there, piece], pair)
                applied_ref[there] += both[:, :r] + both[:, r:]

    def project(slot):
        @pl.when(down[slot])
        def _():
            for copy in onward if slot == XY else left_copies[slot]:
                copy.wait_recv()
            out = None
            for part in (0, 1):
                high, low = split2(left_in[slot, part])
                first = dot32(high, basis_parts[rows(part)])
                term = first[:, :k] + first[:, k:] + dot32(low, basis_parts[rows(part), :k])
                out = term if out is None else out + term
            back_out[slot] = out
            if slot == X:
                pl.when(jnp.logical_not(late))(back_copies[slot].start)
            else:
                back_copies[slot].start()

    late = down[XZ]

    def finish(slot, first, size, *pieces):
        for n in pieces:
            arrived(slot, n)
        apply(slot, pl.ds(first, size))

    finish(Z, 0, m, 0)
    arrived(X, 0)
    pl.when(even)(lambda: start(XY, 0))
    start(XZ, 0)
    arrived(Y, 1)
    start(XY, 1)
    pl.when(jnp.logical_not(late))(lambda: start(XY, 2))
    apply(X, pl.ds(0, half))
    apply(Y, pl.ds(half, half))
    project(Z)
    pl.when(even)(lambda: project(Y))
    pl.when(even)(lambda: finish(XZ, 0, half, 0))
    project(X)
    arrived(X, 1)
    start(XZ, 1)
    arrived(Y, 0)
    apply(X, pl.ds(half, half))

    @pl.when(odd)
    def _():
        start(XY, 0)
        project(Y)

    apply(Y, pl.ds(0, half))
    project(XY)
    pl.when(odd)(lambda: finish(XZ, 0, half, 0))
    pl.when(even)(lambda: finish(XZ, half, half, 1))
    project(XZ)
    pl.when(late)(lambda: start(XY, 2))
    pl.when(jnp.logical_and(late, down[X]))(back_copies[X].start)
    finish(XY, 0, quarter, 0)
    finish(XY, half, quarter, 2)
    pl.when(odd)(lambda: finish(XZ, half, half, 1))
    held = jnp.logical_and(place[2] > 0, even)
    pl.when(jnp.logical_not(held))(lambda: finish(XY, half + quarter, quarter, 3, 4))
    finish(XY, quarter, quarter, 1)
    pl.when(held)(lambda: finish(XY, half + quarter, quarter, 3, 4))
    for s in range(count):
        pl.when(up[s])(back_copies[s].wait_recv)
    for s in range(count):
        for copy, _, flag, _ in sent[s]:
            pl.when(flag)(copy.wait_send)
        for copy in left_copies[s]:
            pl.when(up[s])(copy.wait_send)
        pl.when(down[s])(back_copies[s].wait_send)
    for copy, flag in passed:
        pl.when(flag)(copy[1].wait_send)


def writer(*refs):
    pl.run_scoped(functools.partial(write, *refs), pltpu.SemaphoreType.DMA((2,)))


def write(projected_ref, applied_ref, projected_out, applied_out, sems):
    copies = [
        pltpu.make_async_copy(projected_ref, projected_out, sems.at[0]),
        pltpu.make_async_copy(applied_ref, applied_out, sems.at[1]),
    ]
    for copy in copies:
        copy.start()
    for copy in copies:
        copy.wait()


def solution(mesh):
    sizes = tuple(mesh.shape[name] for name in AXES)

    def local(bases, ranks, couplings, vectors):
        m, k = bases.shape[-2:]
        count = couplings.shape[3]
        r = vectors.shape[-1]
        f32, bf16 = jnp.float32, jnp.bfloat16
        projected, applied = pl.pallas_call(
            functools.partial(kernel, sizes),
            out_shape=(
                pltpu.VMEM((count, k, k), f32),
                pltpu.VMEM((m, r), f32),
            ),
            in_specs=[pl.BlockSpec(memory_space=pltpu.SMEM)] + [pl.BlockSpec(memory_space=pltpu.HBM)] * 3,
            out_specs=(pl.BlockSpec(memory_space=pltpu.VMEM),) * 2,
            scratch_shapes=[
                pltpu.VMEM((m, k), f32),
                pltpu.VMEM((2 * k, m), bf16),
                pltpu.VMEM((m, 2 * k), bf16),
                pltpu.VMEM((count, m, m), bf16),
                pltpu.VMEM((count, m, r), f32),
                pltpu.VMEM((count, 2, k, m // 2), f32),
                pltpu.VMEM((count, 2, k, m // 2), f32),
                pltpu.VMEM((2, k, m // 2), f32),
                pltpu.VMEM((count, k, k), f32),
            ],
            compiler_params=pltpu.CompilerParams(collective_id=0, has_side_effects=True, vmem_limit_bytes=64000 << 10),
        )(
            ranks,
            bases.reshape(m, k),
            couplings.reshape(count, m, m),
            vectors.reshape(m, r),
        )
        projected, applied = pl.pallas_call(
            writer,
            out_shape=(jax.ShapeDtypeStruct(projected.shape, f32), jax.ShapeDtypeStruct(applied.shape, f32)),
            in_specs=[pl.BlockSpec(memory_space=pltpu.VMEM)] * 2,
            out_specs=(pl.BlockSpec(memory_space=pltpu.HBM),) * 2,
            compiler_params=pltpu.CompilerParams(vmem_limit_bytes=8 << 20),
        )(projected, applied)
        return (
            projected.reshape(1, 1, 1, count, k, k),
            applied.reshape(1, 1, 1, m, r),
        )

    return jax.shard_map(
        local,
        mesh=mesh,
        in_specs=(
            P("gx", "gy", "gz", None, None),
            P("gx", "gy", "gz"),
            P("gx", "gy", "gz", None, None, None),
            P("gx", "gy", "gz", None, None),
        ),
        out_specs=(P("gx", "gy", "gz", None, None, None), P("gx", "gy", "gz", None, None)),
        check_vma=False,
    )
```

```python
import functools

import jax
import jax.numpy as jnp
from jax import lax
from jax.experimental import pallas as pl
from jax.experimental.pallas import tpu as pltpu
from jax.sharding import PartitionSpec as P

OFFSET_LIST = ((1, 0, 0), (0, 1, 0), (0, 0, 1), (1, 1, 0), (1, 0, 1), (0, 1, 1), (1, 1, 1))
AXES = ("gx", "gy", "gz")
X, Y, Z, XY, XZ = range(5)
LEFT_ORDER = (XY, Y, X, XZ, Z)


def split2(value):
    high = value.astype(jnp.bfloat16)
    low = (value - high.astype(jnp.float32)).astype(jnp.bfloat16)
    return high, low


def dot32(left, right):
    return jnp.dot(left, right, preferred_element_type=jnp.float32)


def kernel(sizes, *refs):
    dma = pltpu.SemaphoreType.DMA
    count = refs[2].shape[0]
    pl.run_scoped(
        functools.partial(body, sizes, *refs),
        pltpu.SemaphoreType.REGULAR, pltpu.SemaphoreType.REGULAR, dma, dma((count,)), dma((12,)), dma((12,)),
        dma((count + 1,)), dma((count + 1,)), dma((2,)), dma((2,)), dma((count,)), dma((count,)),
    )


def body(
    sizes, ranks_ref, bases_ref, couplings_ref, vectors_ref, projected_ref, applied_ref,
    basis, stacked, basis_parts, blocks, values, left_out, left_in, relay, back_out,
    ready, beyond, basis_sem, block_sem, value_send, value_recv, left_send, left_recv, relay_send, relay_recv,
    back_send, back_recv,
):
    count, m, k = blocks.shape[0], basis.shape[0], basis.shape[1]
    r = applied_ref.shape[1]
    half = m // 2
    place = [lax.axis_index(name) for name in AXES]
    has_up = [p < n - 1 for p, n in zip(place, sizes)]
    has_down = [p > 0 for p in place]

    def every(flags, offset):
        out = None
        for flag, o in zip(flags, offset):
            if o:
                out = flag if out is None else jnp.logical_and(out, flag)
        return out

    up = [every(has_up, o) for o in OFFSET_LIST[:count]]
    down = [every(has_down, o) for o in OFFSET_LIST[:count]]

    def device(offset, sign):
        return {name: p + sign * o for name, p, o in zip(AXES, place, offset)}

    basis_copy = pltpu.make_async_copy(bases_ref, basis, basis_sem)

    even = place[2] % 2 == 0
    odd = jnp.logical_not(even)

    def tell(flag, semaphore, offset, sign):
        @pl.when(flag)
        def _():
            pl.semaphore_signal(
                semaphore, inc=1, device_id=device(offset, sign), device_id_type=pl.DeviceIdType.MESH
            )

    def number(*flags):
        return sum(flag.astype(jnp.int32) for flag in flags)

    def hear(semaphore, amount):
        @pl.when(amount > 0)
        def _():
            pl.semaphore_wait(semaphore, amount)

    barrier = pltpu.get_barrier_semaphore()
    along_x, along_y, along_z = (OFFSET_LIST[s] for s in (X, Y, Z))
    tell(up[X], barrier, along_x, 1)
    tell(up[Y], barrier, along_y, 1)
    tell(jnp.logical_and(odd, up[Z]), barrier, along_z, 1)
    tell(jnp.logical_and(odd, down[Z]), barrier, along_z, -1)
    hear(barrier, number(down[X], down[Y], jnp.logical_and(even, down[Z]), jnp.logical_and(even, up[Z])))

    def rows(part):
        return pl.ds(part * half, half)

    def remote(src, dst, send, recv, offset, sign):
        return pltpu.make_async_remote_copy(
            src_ref=src, dst_ref=dst, send_sem=send, recv_sem=recv,
            device_id=device(offset, sign), device_id_type=pl.DeviceIdType.MESH,
        )

    def value_copy(slot, piece, source, offset):
        n = sum(len(copies) for copies in sent.values())
        return remote(
            source.at[piece], values.at[slot, piece], value_send.at[n], value_recv.at[n], offset, -1,
        )

    sent = {s: [] for s in range(count)}
    quarter, eighth, shift = m // 4, m // 16, m // 64

    def plan(slot, part, source, offset, flag, *cuts):
        for first, size in cuts:
            piece = pl.ds(first, size)
            sent[slot].append((value_copy(slot, piece, source, offset), piece, flag, part))

    for part in (0, 1):
        plan(X, part, vectors_ref, OFFSET_LIST[X], down[X], (part * half, half))
    plan(Y, 0, vectors_ref, OFFSET_LIST[Y], down[Y], (0, half - shift))
    plan(Y, 1, vectors_ref, OFFSET_LIST[Y], down[Y], (half - shift, half + shift))
    plan(Z, 0, vectors_ref, OFFSET_LIST[Z], down[Z], (0, m))
    plan(
        XY, 0, values.at[X], OFFSET_LIST[Y], jnp.logical_and(has_up[0], has_down[1]),
        (0, quarter), (quarter, quarter - shift),
    )
    by_y = jnp.logical_and(has_up[1], has_down[0])
    plan(XY, 1, values.at[Y], OFFSET_LIST[X], by_y, (half - shift, quarter + shift), (half + quarter, quarter - eighth))
    plan(XY, 2, values.at[Y], OFFSET_LIST[X], by_y, (m - eighth, eighth))
    for part in (0, 1):
        plan(
            XZ, part, values.at[X], OFFSET_LIST[Z], jnp.logical_and(has_up[0], has_down[2]), (part * half, half),
        )

    def start(slot, part):
        for copy, _, flag, its in sent[slot]:
            if its == part:
                pl.when(flag)(copy.start)

    def arrived(slot, n):
        pl.when(up[slot])(sent[slot][n][0].wait_recv)

    relays = [
        remote(left_out.at[XY, part], relay.at[part], left_send.at[XY + 2 * part], relay_recv.at[part], OFFSET_LIST[s], 1)
        for part, s in ((0, X), (1, Y))
    ]
    onward = [
        remote(relay.at[part], left_in.at[XY, part], relay_send.at[part], left_recv.at[XY + 2 * part], OFFSET_LIST[s], 1)
        for part, s in ((0, Y), (1, X))
    ]
    passed = (
        ((relays[0], onward[0]), jnp.logical_and(has_down[0], has_up[1])),
        ((relays[1], onward[1]), jnp.logical_and(has_down[1], has_up[0])),
    )
    left_copies = [
        relays if s == XY else [
            remote(left_out.at[s], left_in.at[s], left_send.at[s], left_recv.at[s], OFFSET_LIST[s], 1)
        ]
        for s in range(count)
    ]
    back_copies = [
        remote(back_out.at[s], projected_ref.at[s], back_send.at[s], back_recv.at[s], OFFSET_LIST[s], -1)
        for s in range(count)
    ]

    start(X, 0)
    start(Y, 1)
    basis_copy.start()
    pl.when(even)(lambda: start(Z, 0))
    start(X, 1)
    start(Y, 0)
    tell(down[X], ready, along_x, -1)
    tell(down[Y], ready, along_y, -1)
    tell(jnp.logical_and(even, down[Z]), ready, along_z, -1)
    tell(jnp.logical_and(even, up[Z]), ready, along_z, 1)

    block_copies = [
        pltpu.make_async_copy(couplings_ref.at[s], blocks.at[s], block_sem.at[s]) for s in range(count)
    ]
    for s in LEFT_ORDER:
        block_copies[s].start()

    basis_copy.wait()
    columns = lax.broadcasted_iota(jnp.int32, (m, k), 1)
    masked = jnp.where(columns < ranks_ref[0, 0, 0], basis[...], 0.0)
    high, low = split2(masked)
    basis_parts[:, :k] = high
    basis_parts[:, k:] = low
    high, low = split2(masked.T)
    stacked[:k] = high
    stacked[k:] = low

    hear(ready, number(up[X], up[Y], jnp.logical_and(odd, up[Z]), jnp.logical_and(odd, down[Z])))
    tell(jnp.logical_and(down[Z], up[X]), beyond, along_z, -1)
    pl.when(odd)(lambda: start(Z, 0))

    for s in LEFT_ORDER:
        block_copies[s].wait()

        @pl.when(up[s])
        def _():
            @pl.loop(0, 2)
            def _(part):
                there = pl.ds(pl.multiple_of(part * half, half), half)
                both = dot32(stacked[...], blocks[s, :, there])
                left_out[s, part] = both[:k] + both[k:]

            if s != XZ:
                for copy in left_copies[s]:
                    copy.start()

    applied_ref[...] = jnp.zeros_like(applied_ref)
    for s in range(count):

        @pl.when(jnp.logical_not(up[s]))
        def _():
            projected_ref[s] = jnp.zeros((k, k), jnp.float32)

    for copy, flag in passed:
        @pl.when(flag)
        def _():
            copy[0].wait_recv()
            copy[1].start()

    @pl.when(up[XZ])
    def _():
        pl.semaphore_wait(beyond, 1)
        left_copies[XZ][0].start()

    tall = min(512, m)

    def apply(slot, piece):
        @pl.when(up[slot])
        def _():
            high, low = split2(values[slot, piece])
            pair = jnp.concatenate([high, low], axis=1)

            @pl.loop(0, m // tall)
            def _(step):
                there = pl.ds(pl.multiple_of(step * tall, tall), tall)
                both = dot32(blocks[slot, there, piece], pair)
                applied_ref[there] += both[:, :r] + both[:, r:]

    def project(slot):
        @pl.when(down[slot])
        def _():
            for copy in onward if slot == XY else left_copies[slot]:
                copy.wait_recv()
            out = None
            for part in (0, 1):
                high, low = split2(left_in[slot, part])
                first = dot32(high, basis_parts[rows(part)])
                term = first[:, :k] + first[:, k:] + dot32(low, basis_parts[rows(part), :k])
                out = term if out is None else out + term
            back_out[slot] = out
            if slot == X:
                pl.when(jnp.logical_not(late))(back_copies[slot].start)
            else:
                back_copies[slot].start()

    late = down[XZ]

    def finish(slot, first, size, *pieces):
        for n in pieces:
            arrived(slot, n)
        apply(slot, pl.ds(first, size))

    finish(Z, 0, m, 0)
    arrived(X, 0)
    pl.when(even)(lambda: start(XY, 0))
    start(XZ, 0)
    arrived(Y, 1)
    start(XY, 1)
    pl.when(jnp.logical_not(late))(lambda: start(XY, 2))
    apply(X, pl.ds(0, half))
    apply(Y, pl.ds(half, half))
    project(Z)
    pl.when(even)(lambda: project(Y))
    pl.when(even)(lambda: finish(XZ, 0, half, 0))
    project(X)
    arrived(X, 1)
    start(XZ, 1)
    arrived(Y, 0)
    apply(X, pl.ds(half, half))

    @pl.when(odd)
    def _():
        start(XY, 0)
        project(Y)

    apply(Y, pl.ds(0, half))
    project(XY)
    pl.when(odd)(lambda: finish(XZ, 0, half, 0))
    pl.when(even)(lambda: finish(XZ, half, half, 1))
    project(XZ)
    pl.when(late)(lambda: start(XY, 2))
    pl.when(jnp.logical_and(late, down[X]))(back_copies[X].start)
    finish(XY, 0, quarter, 0)
    finish(XY, half, quarter, 2)
    pl.when(odd)(lambda: finish(XZ, half, half, 1))
    held = jnp.logical_and(place[2] > 0, even)
    pl.when(jnp.logical_not(held))(lambda: finish(XY, half + quarter, quarter, 3, 4))
    finish(XY, quarter, quarter, 1)
    pl.when(held)(lambda: finish(XY, half + quarter, quarter, 3, 4))
    for s in range(count):
        pl.when(up[s])(back_copies[s].wait_recv)
    for s in range(count):
        for copy, _, flag, _ in sent[s]:
            pl.when(flag)(copy.wait_send)
        for copy in left_copies[s]:
            pl.when(up[s])(copy.wait_send)
        pl.when(down[s])(back_copies[s].wait_send)
    for copy, flag in passed:
        pl.when(flag)(copy[1].wait_send)


def writer(*refs):
    pl.run_scoped(functools.partial(write, *refs), pltpu.SemaphoreType.DMA((2,)))


def write(projected_ref, applied_ref, projected_out, applied_out, sems):
    copies = [
        pltpu.make_async_copy(applied_ref, applied_out, sems.at[0]),
        pltpu.make_async_copy(projected_ref, projected_out, sems.at[1]),
    ]
    for copy in copies:
        copy.start()
    for copy in copies:
        copy.wait()


def solution(mesh):
    sizes = tuple(mesh.shape[name] for name in AXES)

    def local(bases, ranks, couplings, vectors):
        m, k = bases.shape[-2:]
        count = couplings.shape[3]
        r = vectors.shape[-1]
        f32, bf16 = jnp.float32, jnp.bfloat16
        projected, applied = pl.pallas_call(
            functools.partial(kernel, sizes),
            out_shape=(
                pltpu.VMEM((count, k, k), f32),
                pltpu.VMEM((m, r), f32),
            ),
            in_specs=[pl.BlockSpec(memory_space=pltpu.SMEM)] + [pl.BlockSpec(memory_space=pltpu.HBM)] * 3,
            out_specs=(pl.BlockSpec(memory_space=pltpu.VMEM),) * 2,
            scratch_shapes=[
                pltpu.VMEM((m, k), f32),
                pltpu.VMEM((2 * k, m), bf16),
                pltpu.VMEM((m, 2 * k), bf16),
                pltpu.VMEM((count, m, m), bf16),
                pltpu.VMEM((count, m, r), f32),
                pltpu.VMEM((count, 2, k, m // 2), f32),
                pltpu.VMEM((count, 2, k, m // 2), f32),
                pltpu.VMEM((2, k, m // 2), f32),
                pltpu.VMEM((count, k, k), f32),
            ],
            compiler_params=pltpu.CompilerParams(collective_id=0, has_side_effects=True, vmem_limit_bytes=64000 << 10),
        )(
            ranks,
            bases.reshape(m, k),
            couplings.reshape(count, m, m),
            vectors.reshape(m, r),
        )
        projected, applied = pl.pallas_call(
            writer,
            out_shape=(jax.ShapeDtypeStruct(projected.shape, f32), jax.ShapeDtypeStruct(applied.shape, f32)),
            in_specs=[pl.BlockSpec(memory_space=pltpu.VMEM)] * 2,
            out_specs=(pl.BlockSpec(memory_space=pltpu.HBM),) * 2,
            compiler_params=pltpu.CompilerParams(vmem_limit_bytes=8 << 20),
        )(projected, applied)
        return (
            projected.reshape(1, 1, 1, count, k, k),
            applied.reshape(1, 1, 1, m, r),
        )

    return jax.shard_map(
        local,
        mesh=mesh,
        in_specs=(
            P("gx", "gy", "gz", None, None),
            P("gx", "gy", "gz"),
            P("gx", "gy", "gz", None, None, None),
            P("gx", "gy", "gz", None, None),
        ),
        out_specs=(P("gx", "gy", "gz", None, None, None), P("gx", "gy", "gz", None, None)),
        check_vma=False,
    )
```
